128 devices in a mesh: dp: 32 (over y, x, core), mp: 4 (over z).
Axes of the slice: x: 4, y: 4, z: 4, core: 2. Of those that a mesh axis runs over, the one named last changes fastest.
Arguments:
- hidden_in: bfloat16 [2, 128, 4096], P(None, 'dp', 'mp'), may hold values from -6 to 6
- rec_gain: float32 [2, 4096], replicated, may hold values from 0.5 to 1.5
- rec_in_x: bfloat16 [2, 4096, 4096], P(None, 'dp', 'mp'), may hold values from -0.09375 to 0.09375
- rec_in_y: bfloat16 [2, 4096, 4096], P(None, 'dp', 'mp'), may hold values from -0.09375 to 0.09375
- conv_weight: float32 [2, 4, 4096], P(None, None, 'mp'), may hold values from -3 to 3
- conv_bias: float32 [2, 4096], P(None, 'mp'), may hold values from -3 to 3
- gate_x_weight: bfloat16 [2, 16, 256, 256], P(None, 'mp'), may hold values from -0.375 to 0.375
- gate_x_bias: float32 [2, 4096], P(None, 'mp'), may hold values from -4 to 4
- gate_a_weight: bfloat16 [2, 16, 256, 256], P(None, 'mp'), may hold values from -0.375 to 0.375
- gate_a_bias: float32 [2, 4096], P(None, 'mp'), may hold values from -4 to 4
- decay_param: float32 [2, 4096], P(None, 'mp'), may hold values from -9 to -1
- rec_out: bfloat16 [2, 4096, 4096], P(None, 'dp', 'mp'), may hold values from -0.09375 to 0.09375
- lru_state: bfloat16 [2, 128, 4096], P(None, 'dp', 'mp'), may hold values from -6 to 6
- conv_state: bfloat16 [2, 3, 128, 4096], P(None, None, 'dp', 'mp'), may hold values from -6 to 6
- scale_index: int32 [2], replicated, may hold values from 0 to 7
- attn_gain: float32 [4096], replicated, may hold values from 0.5 to 1.5
- attn_q: bfloat16 [4096, 4096], P('dp', 'mp'), may hold values from -0.09375 to 0.09375
- attn_kv: bfloat16 [4096, 512], P('dp', 'mp'), may hold values from -0.09375 to 0.09375
- attn_out: bfloat16 [4096, 4096], P('dp', 'mp'), may hold values from -0.09375 to 0.09375
- key_cache: bfloat16 [128, 2048, 256], P('dp', 'mp'), may hold values from -400 to 400
- value_cache: bfloat16 [128, 2048, 256], P('dp', 'mp'), may hold values from -6 to 6
- positions: int32 [128], P('dp'), may hold values from 1 to 6143
Outputs:
- hidden_out: bfloat16 [2, 128, 4096], P(None, 'dp', 'mp')
- lru_out: bfloat16 [2, 128, 4096], P(None, 'dp', 'mp')
- conv_out: bfloat16 [2, 3, 128, 4096], P(None, None, 'dp', 'mp')
- new_kv: bfloat16 [2, 128, 512], P(None, 'dp', 'mp')
The draws below stay inside these ranges and needn't reach their ends.
Inputs may be any that keep to these rules, and one draw needn't show every extreme that they name: `positions`: the count of tokens a sequence has seen; the cache holds its last min(that count, 2048) tokens.
All inputs are finite; a program needn't handle non-finite values.
Results may differ from the reference program's by a relative error of at most 0.03.
Values may be sent and summed in bfloat16 or wider, within the bound.
A program may use at most 64 MiB of HBM per device.

```python
import jax
import jax.numpy as jnp
from jax import lax

D = 4096
LRU = 4096
HEADS = 16
HEAD_DIM = 256
WIN = 2048
CONV = 4
LAYERS = 2
STEPS = 2
BATCH = 128


def draw_key_cache(key, part):
    base = jax.random.normal(jax.random.fold_in(key, 11), (BATCH, WIN, HEAD_DIM), jnp.float32)
    return jnp.clip(base, -400.0, 400.0).astype(jnp.bfloat16)


def plant(entries, key, least, high):
    longest = entries.shape.index(max(entries.shape))
    spots = []
    for shift in (0, 1):
        where = [jax.random.randint(jax.random.fold_in(key, axis), (), 0, length) for axis, length in enumerate(entries.shape)]
        where[longest] = (where[longest] + shift) % entries.shape[longest]
        spots.append(tuple(where))
    return entries.at[spots[0]].set(least).at[spots[1]].set(high)


def shard_levels(own_key, shape, cuts, low, high):
    def one(axis_at, shards_of):
        draws = jax.random.uniform(jax.random.fold_in(jax.random.fold_in(own_key, 6), axis_at), (shards_of,), jnp.float32, low / len(cuts), high / len(cuts))
        return jnp.repeat(jnp.exp(draws), shape[axis_at] // shards_of).reshape((-1,) + (1,) * (len(shape) - axis_at - 1))

    factor_of = one(*cuts[0])
    for cut in cuts[1:]:
        factor_of = factor_of * one(*cut)
    return factor_of


def noise(stream_key, shape, width, bound, pieces=(), held_as=jnp.bfloat16):
    array = jax.random.normal(stream_key, shape, jnp.float32) * width
    if len(pieces) > 0:
        array = shard_levels(stream_key, shape, pieces, -0.22, 0.18) * array
    return jnp.clip(array, min=-bound, max=bound).astype(held_as)


def setup_inputs(seed: int = 0) -> dict:
    key_list = jax.random.split(jax.random.key(seed), 23)
    return {
        "hidden_in": noise(key_list[0], (STEPS, BATCH, D), 1.0, 6.0, ((1, 32), (2, 4))),
        "rec_gain": jnp.clip(1.0 + 0.1 * jax.random.normal(key_list[1], (LAYERS, D), jnp.float32), 0.5, 1.5),
        "rec_in_x": noise(key_list[2], (LAYERS, D, LRU), D ** -0.5, 0.09375, ((1, 32), (2, 4))),
        "rec_in_y": noise(key_list[3], (LAYERS, D, LRU), D ** -0.5, 0.09375, ((1, 32), (2, 4))),
        "conv_weight": noise(key_list[4], (LAYERS, CONV, LRU), 0.5, 3.0, ((2, 4),), jnp.float32),
        "conv_bias": noise(key_list[5], (LAYERS, LRU), 0.5, 3.0, ((1, 4),), jnp.float32),
        "gate_x_weight": noise(key_list[6], (LAYERS, HEADS, LRU // HEADS, LRU // HEADS), (LRU // HEADS) ** -0.5, 0.375, ((1, 4),)),
        "gate_x_bias": noise(key_list[7], (LAYERS, LRU), 1.0, 4.0, ((1, 4),), jnp.float32),
        "gate_a_weight": noise(key_list[8], (LAYERS, HEADS, LRU // HEADS, LRU // HEADS), (LRU // HEADS) ** -0.5, 0.375, ((1, 4),)),
        "gate_a_bias": noise(key_list[9], (LAYERS, LRU), 1.0, 4.0, ((1, 4),), jnp.float32),
        "decay_param": jnp.clip(-9.0 + 8.0 * jax.random.uniform(key_list[10], (LAYERS, LRU), jnp.float32) ** shard_levels(key_list[10], (LAYERS, LRU), ((1, 4),), -0.2, 0.2), -9.0, -1.0),
        "rec_out": noise(key_list[11], (LAYERS, LRU, D), LRU ** -0.5, 0.09375, ((1, 32), (2, 4))),
        "lru_state": noise(key_list[12], (LAYERS, BATCH, LRU), 1.0, 6.0, ((1, 32), (2, 4))),
        "conv_state": noise(key_list[13], (LAYERS, CONV - 1, BATCH, LRU), 1.0, 6.0, ((2, 32), (3, 4))),
        "scale_index": jax.random.randint(key_list[14], (LAYERS,), 0, 8).astype(jnp.int32),
        "attn_gain": jnp.clip(1.0 + 0.1 * jax.random.normal(key_list[15], (D,), jnp.float32), 0.5, 1.5),
        "attn_q": noise(key_list[16], (D, HEADS * HEAD_DIM), D ** -0.5, 0.09375, ((0, 32), (1, 4))),
        "attn_kv": noise(key_list[17], (D, 2 * HEAD_DIM), D ** -0.5, 0.09375, ((0, 32), (1, 4))),
        "attn_out": noise(key_list[18], (HEADS * HEAD_DIM, D), (HEADS * HEAD_DIM) ** -0.5, 0.09375, ((0, 32), (1, 4))),
        "key_cache": draw_key_cache(jax.random.fold_in(key_list[22], 71), 0),
        "value_cache": noise(key_list[20], (BATCH, WIN, HEAD_DIM), 1.0, 6.0, ((0, 32), (1, 4))),
        "positions": plant(jax.random.randint(key_list[21], (BATCH,), 1, 3 * WIN), jax.random.fold_in(key_list[21], 1), 1, (3 * WIN) - 1).astype(jnp.int32),
    }


def norm_rows(values, gain):
    mean_sq = lax.optimization_barrier(jnp.mean(values * values, axis=-1, keepdims=True))
    return (values * lax.rsqrt(mean_sq + 1e-06) * gain.astype(jnp.float32)).astype(jnp.bfloat16)

def lru_gate(filtered_half, weight, bias):
    rows = filtered_half.shape[0]
    shaped = filtered_half.reshape(rows, HEADS, LRU // HEADS).astype(jnp.float32)
    mixed = jnp.einsum('bhi,hij->bhj', shaped, weight.astype(jnp.float32))
    return jax.nn.sigmoid(mixed.reshape(rows, LRU) + bias)

def attend(query, key_cache, value_cache, fresh_keys, fresh_values, positions, step):
    rows = query.shape[0]
    heads = query.reshape(rows, HEADS, HEAD_DIM)

    def single(item):
        head_rows, key_rows, value_rows, new_keys, new_values, position = item
        keys = jnp.concatenate([key_rows, new_keys], 0)
        values = jnp.concatenate([value_rows, new_values], 0)
        scores = jnp.dot(head_rows, keys.T, preferred_element_type=jnp.float32) * HEAD_DIM ** (-0.5)
        slot_ids = jnp.arange(WIN, dtype=jnp.int32)
        held = position - 1 - jnp.mod(position - 1 - slot_ids, WIN)
        cached = (held >= 0) & (held >= position + step - WIN + 1)
        valid = jnp.concatenate([cached, jnp.ones((new_keys.shape[0],), dtype=bool)])
        masked = jnp.where(valid[None, :], scores, -1e+30)
        best = lax.optimization_barrier(jnp.max(masked, axis=-1, keepdims=True))
        weights = jnp.where(valid[None, :], jnp.exp(masked - best), 0.0)
        total = lax.optimization_barrier(jnp.sum(weights, axis=-1, keepdims=True))
        summed = jnp.dot(weights.astype(jnp.bfloat16), values, preferred_element_type=jnp.float32)
        return (summed / total).astype(jnp.bfloat16).reshape(HEADS * HEAD_DIM)
    return lax.map(single, (heads, key_cache, value_cache, fresh_keys, fresh_values, positions))

def reference(hidden_in, rec_gain, rec_in_x, rec_in_y, conv_weight, conv_bias, gate_x_weight, gate_x_bias, gate_a_weight, gate_a_bias, decay_param, rec_out, lru_state, conv_state, scale_index, attn_gain, attn_q, attn_kv, attn_out, key_cache, value_cache, positions):
    scales = 2.0 ** ((scale_index.astype(jnp.float32) - 4.0) * 0.5)
    states = [lru_state[layer].astype(jnp.float32) * scales[layer] for layer in range(LAYERS)]
    windows = [conv_state[layer] for layer in range(LAYERS)]
    fresh_keys = []
    fresh_values = []
    outputs = []
    kv_rows = []
    for step in range(STEPS):
        stream = hidden_in[step].astype(jnp.float32)
        for layer in range(LAYERS):
            normed = norm_rows(stream, rec_gain[layer])
            driven = jnp.dot(normed, rec_in_x[layer], preferred_element_type=jnp.float32).astype(jnp.bfloat16)
            gating = jax.nn.gelu(jnp.dot(normed, rec_in_y[layer], preferred_element_type=jnp.float32), approximate=True)
            taps = jnp.concatenate([windows[layer], driven[None]], 0)
            filtered = lax.optimization_barrier(jnp.sum(taps.astype(jnp.float32) * conv_weight[layer][:, None, :], axis=0)) + conv_bias[layer]
            filtered_half = filtered.astype(jnp.bfloat16)
            input_gate = lru_gate(filtered_half, gate_x_weight[layer], gate_x_bias[layer])
            decay_gate = lru_gate(filtered_half, gate_a_weight[layer], gate_a_bias[layer])
            log_decay = -8.0 * decay_gate * jax.nn.softplus(decay_param[layer])
            states[layer] = jnp.exp(log_decay) * states[layer] + jnp.sqrt(1.0 - jnp.exp(2.0 * log_decay)) * (input_gate * filtered)
            mixed = (states[layer] * gating).astype(jnp.bfloat16)
            stream = stream + jnp.dot(mixed, rec_out[layer], preferred_element_type=jnp.float32)
            windows[layer] = taps[1:]
        normed = norm_rows(stream, attn_gain)
        query = jnp.dot(normed, attn_q, preferred_element_type=jnp.float32).astype(jnp.bfloat16)
        key_value = jnp.dot(normed, attn_kv, preferred_element_type=jnp.float32).astype(jnp.bfloat16)
        kv_rows.append(key_value)
        fresh_keys.append(key_value[:, :HEAD_DIM])
        fresh_values.append(key_value[:, HEAD_DIM:])
        attended = attend(query, key_cache, value_cache, jnp.stack(fresh_keys, 1), jnp.stack(fresh_values, 1), positions, step)
        stream = stream + jnp.dot(attended, attn_out, preferred_element_type=jnp.float32)
        outputs.append(stream.astype(jnp.bfloat16))
    lru_new = jnp.stack([(states[layer] / scales[layer]).astype(jnp.bfloat16) for layer in range(LAYERS)], 0)
    return (jnp.stack(outputs, 0), lru_new, jnp.stack(windows, 0), jnp.stack(kv_rows, 0))
```

```python
import jax
import jax.numpy as jnp
from jax import lax
from jax.experimental import pallas as pl
from jax.experimental.pallas import tpu as pltpu
from jax.sharding import PartitionSpec as P

HEADS = 16
HEAD_DIM = 256
WIN = 2048
LAYERS = 2
STEPS = 2
F32 = jnp.float32
BF16 = jnp.bfloat16
MESH = pl.DeviceIdType.MESH

NDP = 32
NMP = 4
ROWS = 8
SEQ = 4
FEAT = 1024
PIECE = 256
HALF = 512
SLOTS = 512
WIDTHS = (1024, 512, 1024, 512, 640, 512)


def kernel(
    hidden_in,
    rec_gain,
    rec_in_x,
    rec_in_y,
    conv_weight,
    conv_bias,
    gate_x_weight,
    gate_x_bias,
    gate_a_weight,
    gate_a_bias,
    decay_param,
    rec_out,
    lru_state,
    conv_state,
    scale_index,
    attn_gain,
    attn_q,
    attn_kv,
    attn_out,
    key_cache,
    value_cache,
    positions,
    hidden_out,
    lru_out,
    conv_out,
    new_kv,
    hid_v,
    rgain_v,
    again_v,
    cw_v,
    cb_v,
    gxw_v,
    gxb_v,
    gaw_v,
    gab_v,
    dec_v,
    lru_v,
    conv_v,
    key_v,
    val_v,
    wkv_v,
    win0,
    win1,
    wout0,
    wout1,
    wq,
    wo,
    scale_s,
    pos_s,
    x_v,
    f8,
    st_v,
    t0_v,
    t1_v,
    t2_v,
    mask_v,
    asend,
    abuf,
    bs0,
    bs1,
    bs2,
    bs3,
    bs4,
    bs5,
    bb0,
    bb1,
    bb2,
    bb3,
    bb4,
    bb5,
    nsend,
    nbuf,
    zsend,
    zbuf,
    csend,
    cbuf,
    tsend,
    tbuf,
    lsem,
    wsend,
    wrecv,
    asnd,
    arcv,
    bsnd,
    brcv,
    nsnd,
    nrcv,
    zsnd,
    zrcv,
    csnd,
    crcv,
    tsnd,
    trcv,
):
    i = lax.axis_index("dp")
    j = lax.axis_index("mp")
    core = lax.rem(i, 2)
    mate = i + 1 - 2 * core
    yy = lax.div(i, 8)
    xx = lax.div(lax.rem(i, 8), 2)
    bsend = (bs0, bs1, bs2, bs3, bs4, bs5)
    bbuf = (bb0, bb1, bb2, bb3, bb4, bb5)

    def local(src, dst, k):
        copy = pltpu.make_async_copy(src, dst, lsem.at[k])
        copy.start()
        return copy

    fcol = pl.ds(pl.multiple_of(j * FEAT, FEAT), FEAT)
    mine = pl.ds(pl.multiple_of(core * HALF, HALF), HALF)
    other = pl.ds(pl.multiple_of((1 - core) * HALF, HALF), HALF)
    krow = pl.ds(pl.multiple_of(core * 128, 128), 128)

    c_hid = local(hidden_in, hid_v, 0)
    c_rg = local(rec_gain.at[:, fcol], rgain_v, 1)

    barrier = pltpu.get_barrier_semaphore()

    def greet_plane(k, _):
        @pl.when(jnp.logical_not((k == i) & (yy == j)))
        def _():
            pl.semaphore_signal(barrier, inc=1, device_id=(k, yy), device_id_type=MESH)

        return 0

    lax.fori_loop(0, NDP, greet_plane, 0)

    def greet_dp(k, _):
        pl.semaphore_signal(
            barrier, inc=1, device_id=(lax.rem(i + k, NDP), j), device_id_type=MESH
        )
        return 0

    lax.fori_loop(1, NDP, greet_dp, 0)

    def greet_mp(k, _):
        pl.semaphore_signal(
            barrier, inc=1, device_id=(i, lax.rem(j + k, NMP)), device_id_type=MESH
        )
        return 0

    lax.fori_loop(1, NMP, greet_mp, 0)

    weights = (
        (rec_in_x.at[0], win0, 0),
        (rec_in_y.at[0], win0, HALF),
        (rec_out.at[0], wout0, 0),
        (rec_in_x.at[1], win1, 0),
        (rec_in_y.at[1], win1, HALF),
        (rec_out.at[1], wout1, 0),
        (attn_q, wq, 0),
        (attn_out, wo, 0),
    )
    c_w = [
        local(src.at[:, mine], dst.at[krow, pl.ds(at, HALF)], 2 + k)
        for k, (src, dst, at) in enumerate(weights)
    ]
    c_lru = local(lru_state, lru_v, 10)
    c_conv = local(conv_state, conv_v, 11)
    c_sc = local(scale_index, scale_s, 12)
    c_pos = local(positions, pos_s, 13)
    c_cw = local(conv_weight, cw_v, 14)
    c_cb = local(conv_bias, cb_v, 15)
    c_gxb = local(gate_x_bias, gxb_v, 16)
    c_gab = local(gate_a_bias, gab_v, 17)
    c_dec = local(decay_param, dec_v, 18)
    c_gxw = local(gate_x_weight, gxw_v, 19)
    c_gaw = local(gate_a_weight, gaw_v, 20)
    c_ag = local(attn_gain.at[:, fcol], again_v, 21)
    c_wkv = local(attn_kv, wkv_v, 22)
    c_key = local(key_cache, key_v, 23)
    c_val = local(value_cache, val_v, 24)

    row = lax.broadcasted_iota(jnp.int32, (ROWS, FEAT), 0)
    late = row >= SEQ

    def norm_send(k):
        x = x_v[...]
        sq = jnp.sum(x * x, axis=-1, keepdims=True)
        sq = jnp.broadcast_to(sq, (ROWS, 128))
        nsend[k] = sq
        nbuf[k, j] = sq

        def one(d, _):
            pltpu.make_async_remote_copy(
                src_ref=nsend.at[k],
                dst_ref=nbuf.at[k, j],
                send_sem=nsnd.at[k],
                recv_sem=nrcv.at[k],
                device_id=(i, lax.rem(j + d, NMP)),
                device_id_type=MESH,
            ).start()
            return 0

        lax.fori_loop(1, NMP, one, 0)

    def norm_scale(k):
        view = nbuf.at[k, pl.ds(0, NMP - 1)]
        pltpu.make_async_copy(view, view, nrcv.at[k]).wait()
        total = (nbuf[k, 0] + nbuf[k, 1]) + (nbuf[k, 2] + nbuf[k, 3])
        return lax.rsqrt(total[:, :1] * (1.0 / 4096.0) + 1e-06)

    def spread(k):
        def one(n, _):
            q = lax.div(n, NMP)
            z = lax.rem(n, NMP)
            d = 8 * j + q

            @pl.when(jnp.logical_not((d == i) & (z == j)))
            def _():
                pltpu.make_async_remote_copy(
                    src_ref=asend.at[k, lax.div(q, 2)],
                    dst_ref=abuf.at[k, i],
                    send_sem=asnd.at[k],
                    recv_sem=arcv.at[k],
                    device_id=(d, z),
                    device_id_type=MESH,
                ).start()

            return 0

        lax.fori_loop(0, NDP, one, 0)

        @pl.when(yy == j)
        def _():
            abuf[k, i] = asend[k, xx]

    def spread_wait(k):
        @pl.when(yy == j)
        def _():
            view = abuf.at[k, pl.ds(0, NDP - 1)]
            pltpu.make_async_copy(view, view, arcv.at[k]).wait()

        @pl.when(yy != j)
        def _():
            view = abuf.at[k]
            pltpu.make_async_copy(view, view, arcv.at[k]).wait()

    def arrived(k):
        spread_wait(k)
        return abuf[k].astype(F32).reshape(NDP * ROWS, PIECE).astype(BF16)

    def project(k, act, weight, width):
        for n in range(width // PIECE):
            cols = slice(n * PIECE, (n + 1) * PIECE)
            part = jnp.dot(act, weight[:, cols], preferred_element_type=F32)
            bsend[k][:, :, cols] = part.reshape(NDP, ROWS, PIECE).astype(BF16)

    def reduce_send(k):
        def one(n, _):
            d = lax.rem(i + n, NDP)
            pltpu.make_async_remote_copy(
                src_ref=bsend[k].at[d],
                dst_ref=bbuf[k].at[i],
                send_sem=bsnd.at[k],
                recv_sem=brcv.at[k],
                device_id=(d, j),
                device_id_type=MESH,
            ).start()
            return 0

        lax.fori_loop(1, NDP, one, 0)
        bbuf[k][i] = bsend[k][i]

    def reduce_wait(k):
        view = bbuf[k].at[pl.ds(0, NDP - 1)]
        pltpu.make_async_copy(view, view, brcv.at[k]).wait()

    def summed(k, c, cols):
        acc = bbuf[k][c, :, cols].astype(F32)
        for p in range(1, NDP // 2):
            acc = acc + bbuf[k][2 * p + c, :, cols].astype(F32)
        return acc

    def set_pieces(k, values):
        for q in range(NMP):
            asend[k, q] = values[:, q * PIECE : (q + 1) * PIECE].astype(BF16)

    c_hid.wait()
    c_rg.wait()
    x_v[0:SEQ, :] = hid_v[0].astype(F32)
    x_v[SEQ:ROWS, :] = hid_v[1].astype(F32)
    set_pieces(0, x_v[...] * rgain_v[0:1, :])

    met = 2 * NDP - 1 + NMP - 1
    pl.semaphore_wait(barrier, jnp.where(yy == j, met - 1, met))

    spread(0)
    w_out = [
        pltpu.make_async_remote_copy(
            src_ref=src.at[:, other],
            dst_ref=dst.at[krow, pl.ds(at, HALF)],
            send_sem=wsend.at[k],
            recv_sem=wrecv.at[k],
            device_id=(mate, j),
            device_id_type=MESH,
        )
        for k, (src, dst, at) in enumerate(weights)
    ]
    for copy in w_out:
        copy.start()
    norm_send(0)

    c_lru.wait()
    c_conv.wait()
    c_sc.wait()
    scales = []
    for l in range(LAYERS):
        power = (scale_s[l].astype(F32) - 4.0) * 0.5
        scales.append(jnp.exp2(jnp.full((1, 128), power, F32))[:, :1])
        st_v[l, 0:SEQ, :] = lru_v[l].astype(F32) * scales[l]
        st_v[l, SEQ:ROWS, :] = jnp.zeros((SEQ, FEAT), F32)
        w0 = conv_v[l, 0].astype(F32)
        w1 = conv_v[l, 1].astype(F32)
        w2 = conv_v[l, 2].astype(F32)
        t0_v[l, 0:SEQ, :] = w0
        t0_v[l, SEQ:ROWS, :] = w1
        t1_v[l, 0:SEQ, :] = w1
        t1_v[l, SEQ:ROWS, :] = w2
        t2_v[l, 0:SEQ, :] = w2
        t2_v[l, SEQ:ROWS, :] = jnp.zeros((SEQ, FEAT), F32)
        conv_out[l, 0] = conv_v[l, 2]
    c_pos.wait()
    srow = lax.broadcasted_iota(jnp.int32, (ROWS, SLOTS), 0)
    slot = lax.broadcasted_iota(jnp.int32, (ROWS, SLOTS), 1) + j * SLOTS
    seq = srow & 3
    pos = jnp.where(
        seq == 0, pos_s[0], jnp.where(seq == 1, pos_s[1], jnp.where(seq == 2, pos_s[2], pos_s[3]))
    )
    step = lax.shift_right_logical(srow, 2)
    held = pos - 1 - ((pos - 1 - slot) & (WIN - 1))
    mask_v[...] = jnp.where((held >= 0) & (held >= pos + step - (WIN - 1)), 1.0, 0.0).astype(F32)
    for copy in (c_cw, c_cb, c_gxb, c_gab, c_dec, c_gxw, c_gaw):
        copy.wait()

    def recurrent(l):
        ka, kb = 2 * l, 2 * l + 1
        weight = (win0, win1)[l]
        for k in (3 * l, 3 * l + 1):
            c_w[k].wait()
            w_out[k].wait_recv()
        act = arrived(ka)
        project(ka, act, weight, 2 * HALF)
        reduce_send(ka)
        scale = norm_scale(l)
        decay = dec_v[l : l + 1, :]
        soft = jnp.maximum(decay, 0.0) + jnp.log1p(jnp.exp(-jnp.abs(decay)))
        partial_taps = (
            cw_v[l, 0:1, :] * t0_v[l] + cw_v[l, 1:2, :] * t1_v[l] + cb_v[l : l + 1, :]
        )
        reduce_wait(ka)
        for c in range(2):
            cols = slice(c * HALF, (c + 1) * HALF)
            u = summed(ka, c, slice(0, HALF)) * scale
            f8[0, :, cols] = u.astype(BF16).astype(F32)
            f8[1, :, cols] = summed(ka, c, slice(HALF, 2 * HALF)) * scale
        u = f8[0]
        v = f8[1]
        u_roll = pltpu.roll(u, SEQ, 0)
        conv_out[l, 1] = u[0:SEQ].astype(BF16)
        conv_out[l, 2] = u_roll[0:SEQ].astype(BF16)
        t2 = jnp.where(late, u_roll, t2_v[l])
        filtered = partial_taps + cw_v[l, 2:3, :] * t2 + cw_v[l, 3:4, :] * u
        half = filtered.astype(BF16)
        for b in range(4):
            cols = slice(b * PIECE, (b + 1) * PIECE)
            f8[2, :, cols] = jnp.dot(half[:, cols], gxw_v[l, b], preferred_element_type=F32)
            f8[3, :, cols] = jnp.dot(half[:, cols], gaw_v[l, b], preferred_element_type=F32)
        gi = 1.0 / (1.0 + jnp.exp(-(f8[2] + gxb_v[l : l + 1, :])))
        ga = 1.0 / (1.0 + jnp.exp(-(f8[3] + gab_v[l : l + 1, :])))
        log_a = -8.0 * ga * soft
        a = jnp.exp(log_a)
        add = jnp.sqrt(1.0 - jnp.exp(2.0 * log_a)) * (gi * filtered)
        first = a * st_v[l] + add
        second = a * pltpu.roll(first, SEQ, 0) + add
        state = jnp.where(late, second, first)
        gelu = 0.5 * v * (1.0 + jnp.tanh(0.7978845608028654 * (v + 0.044715 * (v * v * v))))
        set_pieces(kb, state * gelu)
        spread(kb)
        lru_out[l] = (pltpu.roll(state, SEQ, 0)[0:SEQ] / scales[l]).astype(BF16)

        k = 3 * l + 2
        c_w[k].wait()
        w_out[k].wait_recv()
        act = arrived(kb)
        project(kb, act, (wout0, wout1)[l], HALF)
        reduce_send(kb)
        reduce_wait(kb)
        for c in range(2):
            cols = slice(c * HALF, (c + 1) * HALF)
            x_v[:, cols] = x_v[:, cols] + summed(kb, c, slice(0, HALF))

    recurrent(0)
    set_pieces(2, x_v[...] * rgain_v[1:2, :])
    spread(2)
    norm_send(1)
    recurrent(1)
    c_ag.wait()
    set_pieces(4, x_v[...] * again_v[...])
    spread(4)
    norm_send(2)

    for copy in (c_wkv, c_key, c_val, c_w[6], c_w[7]):
        copy.wait()
    w_out[6].wait_recv()
    act = arrived(4)
    project(4, act, wq, HALF)
    own = pl.ds(pl.multiple_of(core * 128, 128), 128)
    act = abuf[4, :, :, own].astype(F32).reshape(NDP * ROWS, 128).astype(BF16)
    part = jnp.dot(act, wkv_v[...], preferred_element_type=F32)
    bs4[:, :, HALF:] = part.reshape(NDP, ROWS, 128).astype(BF16)
    reduce_send(4)
    scale = norm_scale(2)
    reduce_wait(4)
    for c in range(2):
        zsend[:, c * HALF : (c + 1) * HALF] = (summed(4, c, slice(0, HALF)) * scale).astype(BF16)
    kv = (summed(4, 0, slice(HALF, HALF + 128)) + summed(4, 1, slice(HALF, HALF + 128))) * scale
    zsend[:, FEAT:] = kv.astype(BF16)

    def query_send(d, _):
        pltpu.make_async_remote_copy(
            src_ref=zsend,
            dst_ref=zbuf.at[j],
            send_sem=zsnd,
            recv_sem=zrcv,
            device_id=(i, lax.rem(j + d, NMP)),
            device_id_type=MESH,
        ).start()
        return 0

    lax.fori_loop(1, NMP, query_send, 0)
    zbuf[j] = zsend[...]
    new_kv[0] = kv[0:SEQ].astype(BF16)
    new_kv[1] = pltpu.roll(kv, SEQ, 0)[0:SEQ].astype(BF16)
    view = zbuf.at[pl.ds(0, NMP - 1)]
    pltpu.make_async_copy(view, view, zrcv).wait()

    rows = HEADS * ROWS
    query = jnp.concatenate(
        [
            zbuf[z, :, h * HEAD_DIM : (h + 1) * HEAD_DIM].astype(F32)
            for z in range(NMP)
            for h in range(HEADS // NMP)
        ],
        axis=0,
    ).astype(BF16)
    which = lax.broadcasted_iota(jnp.int32, (rows, SLOTS), 0) & 3
    scores = None
    for b in range(SEQ):
        one = lax.dot_general(
            query, key_v[b], (((1,), (1,)), ((), ())), preferred_element_type=F32
        )
        scores = one if scores is None else jnp.where(which == b, one, scores)
    mask = jnp.broadcast_to(mask_v[...][None], (HEADS, ROWS, SLOTS)).reshape(rows, SLOTS)
    scores = jnp.where(mask > 0.5, scores * HEAD_DIM ** (-0.5), -1e30)
    top = jnp.max(scores, axis=-1, keepdims=True)
    weight = jnp.exp(scores - top) * mask
    total = jnp.sum(weight, axis=-1, keepdims=True)
    values = None
    for b in range(SEQ):
        one = jnp.dot(
            jnp.where(which == b, weight, 0.0).astype(BF16), val_v[b], preferred_element_type=F32
        )
        values = one if values is None else values + one
    lane = lax.broadcasted_iota(jnp.int32, (rows, 128), 1)
    csend[...] = values.reshape(HEADS, ROWS, HEAD_DIM).astype(BF16)
    tsend[...] = jnp.where(lane < 64, top, total).reshape(HEADS, ROWS, 128)

    def part_send(d, _):
        z = lax.rem(j + d, NMP)
        group = pl.ds(4 * z, 4)
        pltpu.make_async_remote_copy(
            src_ref=csend.at[group],
            dst_ref=cbuf.at[j],
            send_sem=csnd,
            recv_sem=crcv,
            device_id=(i, z),
            device_id_type=MESH,
        ).start()
        pltpu.make_async_remote_copy(
            src_ref=tsend.at[group],
            dst_ref=tbuf.at[j],
            send_sem=tsnd,
            recv_sem=trcv,
            device_id=(i, z),
            device_id_type=MESH,
        ).start()
        return 0

    lax.fori_loop(1, NMP, part_send, 0)
    cbuf[j] = csend[pl.ds(4 * j, 4)]
    tbuf[j] = tsend[pl.ds(4 * j, 4)]

    lateh = lax.broadcasted_iota(jnp.int32, (ROWS, HEAD_DIM), 0) >= SEQ
    late1 = lax.broadcasted_iota(jnp.int32, (ROWS, 1), 0) >= SEQ

    def pair(lo, hi):
        at = slice(FEAT, FEAT + 128)
        both = jnp.concatenate([zbuf[lo, :, at].astype(F32), zbuf[hi, :, at].astype(F32)], axis=1)
        turned = pltpu.roll(both, SEQ, 0)
        return jnp.where(lateh, turned, both), jnp.where(lateh, both, turned)

    key0, key1 = pair(0, 1)
    val0, val1 = pair(2, 3)
    fresh = []
    for h in range(4):
        head = zsend[:, h * HEAD_DIM : (h + 1) * HEAD_DIM].astype(F32)
        s0 = jnp.sum(head * key0, axis=-1, keepdims=True) * HEAD_DIM ** (-0.5)
        s1 = jnp.sum(head * key1, axis=-1, keepdims=True) * HEAD_DIM ** (-0.5)
        fresh.append((s0, jnp.where(late1, s1, -1e30)))
    view = cbuf.at[pl.ds(0, NMP - 1)]
    pltpu.make_async_copy(view, view, crcv).wait()
    view = tbuf.at[pl.ds(0, NMP - 1)]
    pltpu.make_async_copy(view, view, trcv).wait()
    for h in range(4):
        s0, s1 = fresh[h]
        tops = [tbuf[z, h, :, 0:1] for z in range(NMP)]
        best = jnp.maximum(s0, s1)
        for t in tops:
            best = jnp.maximum(best, t)
        w0 = jnp.exp(s0 - best)
        w1 = jnp.where(late1, jnp.exp(s1 - best), 0.0)
        den = w0 + w1
        num = w0.astype(BF16).astype(F32) * val0 + w1.astype(BF16).astype(F32) * val1
        for z in range(NMP):
            fade = jnp.exp(tops[z] - best)
            den = den + fade * tbuf[z, h, :, 64:65]
            num = num + fade * cbuf[z, h].astype(F32)
        asend[5, h] = (num / den).astype(BF16)
    spread(5)
    w_out[7].wait_recv()
    act = arrived(5)
    project(5, act, wo, HALF)
    reduce_send(5)
    reduce_wait(5)
    for c in range(2):
        cols = slice(c * HALF, (c + 1) * HALF)
        x_v[:, cols] = x_v[:, cols] + summed(5, c, slice(0, HALF))
    x = x_v[...]
    hidden_out[0] = x[0:SEQ].astype(BF16)
    hidden_out[1] = pltpu.roll(x, SEQ, 0)[0:SEQ].astype(BF16)

    for copy in w_out:
        copy.wait_send()
    for k in range(3):
        view = nbuf.at[k, pl.ds(0, NMP - 1)]
        pltpu.make_async_copy(view, view, nsnd.at[k]).wait()
    for k in range(6):
        view = bbuf[k].at[pl.ds(0, NDP - 1)]
        pltpu.make_async_copy(view, view, bsnd.at[k]).wait()

        @pl.when(yy == j)
        def _():
            view = abuf.at[k, pl.ds(0, NDP - 1)]
            pltpu.make_async_copy(view, view, asnd.at[k]).wait()

        @pl.when(yy != j)
        def _():
            view = abuf.at[k]
            pltpu.make_async_copy(view, view, asnd.at[k]).wait()

    for buf, sem in ((zbuf, zsnd), (cbuf, csnd), (tbuf, tsnd)):
        view = buf.at[pl.ds(0, NMP - 1)]
        pltpu.make_async_copy(view, view, sem).wait()


def body(*args):
    args = list(args)
    args[15] = args[15].reshape(1, -1)
    shape = jax.ShapeDtypeStruct
    hbm = pl.BlockSpec(memory_space=pl.ANY)
    vmem = pl.BlockSpec(memory_space=pltpu.VMEM)
    V = pltpu.VMEM
    DMA = pltpu.SemaphoreType.DMA
    scratch = [
        V((STEPS, SEQ, FEAT), BF16),
        V((LAYERS, FEAT), F32),
        V((1, FEAT), F32),
        V((LAYERS, 4, FEAT), F32),
        V((LAYERS, FEAT), F32),
        V((LAYERS, 4, PIECE, PIECE), BF16),
        V((LAYERS, FEAT), F32),
        V((LAYERS, 4, PIECE, PIECE), BF16),
        V((LAYERS, FEAT), F32),
        V((LAYERS, FEAT), F32),
        V((LAYERS, SEQ, FEAT), BF16),
        V((LAYERS, 3, SEQ, FEAT), BF16),
        V((SEQ, SLOTS, HEAD_DIM), BF16),
        V((SEQ, SLOTS, HEAD_DIM), BF16),
        V((128, 128), BF16),
        V((PIECE, 2 * HALF), BF16),
        V((PIECE, 2 * HALF), BF16),
        V((PIECE, HALF), BF16),
        V((PIECE, HALF), BF16),
        V((PIECE, HALF), BF16),
        V((PIECE, HALF), BF16),
        pltpu.SMEM((LAYERS,), jnp.int32),
        pltpu.SMEM((SEQ,), jnp.int32),
        V((ROWS, FEAT), F32),
        V((4, ROWS, FEAT), F32),
        V((LAYERS, ROWS, FEAT), F32),
        V((LAYERS, ROWS, FEAT), F32),
        V((LAYERS, ROWS, FEAT), F32),
        V((LAYERS, ROWS, FEAT), F32),
        V((ROWS, SLOTS), F32),
        V((6, NMP, ROWS, PIECE), BF16),
        V((6, NDP, ROWS, PIECE), BF16),
        *[V((NDP, ROWS, w), BF16) for w in WIDTHS],
        *[V((NDP, ROWS, w), BF16) for w in WIDTHS],
        V((3, ROWS, 128), F32),
        V((3, NMP, ROWS, 128), F32),
        V((ROWS, FEAT + 128), BF16),
        V((NMP, ROWS, FEAT + 128), BF16),
        V((HEADS, ROWS, HEAD_DIM), BF16),
        V((NMP, 4, ROWS, HEAD_DIM), BF16),
        V((HEADS, ROWS, 128), F32),
        V((NMP, 4, ROWS, 128), F32),
        DMA((25,)),
        DMA((8,)),
        DMA((8,)),
        DMA((6,)),
        DMA((6,)),
        DMA((6,)),
        DMA((6,)),
        DMA((3,)),
        DMA((3,)),
        DMA,
        DMA,
        DMA,
        DMA,
        DMA,
        DMA,
    ]
    return pl.pallas_call(
        kernel,
        out_shape=(
            shape((STEPS, SEQ, FEAT), BF16),
            shape((LAYERS, SEQ, FEAT), BF16),
            shape((LAYERS, 3, SEQ, FEAT), BF16),
            shape((STEPS, SEQ, 128), BF16),
        ),
        in_specs=[hbm] * 22,
        out_specs=(vmem,) * 4,
        scratch_shapes=scratch,
        compiler_params=pltpu.CompilerParams(
            collective_id=0, has_side_effects=True, vmem_limit_bytes=40 * 1024 * 1024
        ),
    )(*args)


def solution(mesh):
    placed = (
        P(None, "dp", "mp"),
        P(),
        P(None, "dp", "mp"),
        P(None, "dp", "mp"),
        P(None, None, "mp"),
        P(None, "mp"),
        P(None, "mp", None, None),
        P(None, "mp"),
        P(None, "mp", None, None),
        P(None, "mp"),
        P(None, "mp"),
        P(None, "dp", "mp"),
        P(None, "dp", "mp"),
        P(None, None, "dp", "mp"),
        P(),
        P(),
        P("dp", "mp"),
        P("dp", "mp"),
        P("dp", "mp"),
        P("dp", "mp", None),
        P("dp", "mp", None),
        P("dp"),
    )
    return jax.shard_map(
        body,
        mesh=mesh,
        in_specs=placed,
        out_specs=(
            P(None, "dp", "mp"),
            P(None, "dp", "mp"),
            P(None, None, "dp", "mp"),
            P(None, "dp", "mp"),
        ),
        check_vma=False,
    )
```

```python
import jax
import jax.numpy as jnp
from jax import lax
from jax.experimental import pallas as pl
from jax.experimental.pallas import tpu as pltpu
from jax.sharding import PartitionSpec as P

HEADS = 16
HEAD_DIM = 256
WIN = 2048
LAYERS = 2
STEPS = 2
F32 = jnp.float32
BF16 = jnp.bfloat16
MESH = pl.DeviceIdType.MESH

NDP = 32
NMP = 4
NX = 4
ROWS = 8
SEQ = 4
FEAT = 1024
PIECE = 256
HALF = 512
SLOTS = 512
BLOCKS = 8
BLOCK = 32
CHIPS = 16
VMEM = 67043328


def scratch_list():
    V = pltpu.VMEM
    DMA = pltpu.SemaphoreType.DMA
    return [
        ("hid_v", V((STEPS, SEQ, FEAT), BF16)),
        ("rgain_v", V((2, LAYERS, PIECE), F32)),
        ("again_v", V((1, PIECE), F32)),
        ("cw_v", V((LAYERS, 4, PIECE), F32)),
        ("cb_v", V((LAYERS, PIECE), F32)),
        ("gxw_v", V((LAYERS, PIECE, PIECE), BF16)),
        ("gxb_v", V((LAYERS, PIECE), F32)),
        ("gaw_v", V((LAYERS, PIECE, PIECE), BF16)),
        ("gab_v", V((LAYERS, PIECE), F32)),
        ("dec_v", V((LAYERS, PIECE), F32)),
        ("win_v", V((LAYERS, 3, SEQ, FEAT), BF16)),
        ("key_v", V((SEQ, SLOTS, HEAD_DIM), BF16)),
        ("val_v", V((SEQ, SLOTS, HEAD_DIM), BF16)),
        ("wkv_v", V((128, 128), BF16)),
        ("wi", V((LAYERS, PIECE, 2 * HALF), BF16)),
        ("wr", V((LAYERS, PIECE, HALF), BF16)),
        ("wq", V((PIECE, HALF), BF16)),
        ("wo", V((PIECE, HALF), BF16)),
        ("scale_s", pltpu.SMEM((LAYERS,), jnp.int32)),
        ("pos_s", pltpu.SMEM((SEQ,), jnp.int32)),
        ("x_v", V((NX, ROWS, PIECE), F32)),
        ("h_v", V((ROWS, FEAT), F32)),
        ("st_v", V((LAYERS, NX, ROWS, PIECE), F32)),
        ("t0_v", V((LAYERS, NX, ROWS, PIECE), F32)),
        ("t1_v", V((LAYERS, NX, ROWS, PIECE), F32)),
        ("t2_v", V((LAYERS, NX, ROWS, PIECE), F32)),
        ("mask_v", V((ROWS, SLOTS), F32)),
        ("lru_b", V((NX, LAYERS, SEQ, PIECE), BF16)),
        ("win_b", V((NX, LAYERS, 3, SEQ, PIECE), BF16)),
        ("lru_s", V((LAYERS, NX, SEQ, PIECE), BF16)),
        ("win_s", V((LAYERS, NX, 2, SEQ, PIECE), BF16)),
        ("pieces", V((2, NMP, ROWS, PIECE), BF16)),
        ("spread_b", V((2, 2, CHIPS, ROWS, PIECE), BF16)),
        ("act_s", V((4, BLOCK, PIECE), BF16)),
        ("act_b", V((4, 2, 4, BLOCK, PIECE), BF16)),
        ("in_s", V((LAYERS, 2, BLOCKS, BLOCK, HALF), BF16)),
        ("in_b", V((LAYERS, CHIPS, BLOCK, HALF), BF16)),
        ("out_s", V((LAYERS, 2, BLOCKS, BLOCK, PIECE), BF16)),
        ("out_b", V((LAYERS, CHIPS, BLOCK, PIECE), BF16)),
        ("q_s", V((NDP, ROWS, HALF + 128), BF16)),
        ("q_b", V((NDP, ROWS, HALF + 128), BF16)),
        ("o_s", V((NDP, ROWS, HALF), BF16)),
        ("o_b", V((NDP, ROWS, HALF), BF16)),
        ("ent_b", V((NX, ROWS, PIECE), BF16)),
        ("res_s", V((NX, ROWS, PIECE), F32)),
        ("res_b", V((NX, ROWS, PIECE), F32)),
        ("nsend", V((3, 1, 128), F32)),
        ("nbuf", V((3, CHIPS, 1, 128), F32)),
        ("zsend", V((ROWS, FEAT + 128), BF16)),
        ("zbuf", V((NMP, ROWS, FEAT + 128), BF16)),
        ("csend", V((HEADS, ROWS, HEAD_DIM), BF16)),
        ("cbuf", V((NMP, 4, ROWS, HEAD_DIM), BF16)),
        ("tsend", V((HEADS, ROWS, 128), F32)),
        ("tbuf", V((NMP, 4, ROWS, 128), F32)),
        ("lsem", DMA((32,))),
        ("snd", DMA((48,))),
        ("rcv", DMA((48,))),
    ]


NAMES = (
    "hidden_in",
    "rec_gain",
    "rec_in_x",
    "rec_in_y",
    "conv_weight",
    "conv_bias",
    "gate_x_weight",
    "gate_x_bias",
    "gate_a_weight",
    "gate_a_bias",
    "decay_param",
    "rec_out",
    "lru_state",
    "conv_state",
    "scale_index",
    "attn_gain",
    "attn_q",
    "attn_kv",
    "attn_out",
    "key_cache",
    "value_cache",
    "positions",
    "hidden_out",
    "lru_out",
    "conv_out",
    "new_kv",
)


class Refs:
    def __init__(self, refs):
        names = (*NAMES, *(name for name, _ in scratch_list()))
        for name, ref in zip(names, refs, strict=True):
            setattr(self, name, ref)


def kernel(*refs):
    r = Refs(refs)
    i = lax.axis_index("dp")
    j = lax.axis_index("mp")
    core = lax.rem(i, 2)
    mate = i + 1 - 2 * core
    yy = lax.div(i, 8)
    xx = lax.div(lax.rem(i, 8), 2)
    diagonal = yy == j
    inside = lax.div(xx, 2) == core

    pending = {}
    used = [0, 0]

    def take(*names):
        for name in names:
            pending.pop(name)()

    def sems():
        used[1] += 1
        assert used[1] <= 48
        return r.snd.at[used[1] - 1], r.rcv.at[used[1] - 1]

    def local(name, src, dst):
        sem = r.lsem.at[used[0]]
        used[0] += 1
        copy = pltpu.make_async_copy(src, dst, sem)
        copy.start()
        pending[name] = copy.wait

    def remote(src, dst, pair, device):
        pltpu.make_async_remote_copy(
            src_ref=src,
            dst_ref=dst,
            send_sem=pair[0],
            recv_sem=pair[1],
            device_id=device,
            device_id_type=MESH,
        ).start()

    def bytes_of(view, sem):
        return lambda: pltpu.make_async_copy(view, view, sem).wait()

    def all_but_self(buf, sem, own):
        def wait():
            @pl.when(own)
            def _():
                bytes_of(buf.at[pl.ds(0, buf.shape[0] - 1)], sem)()

            @pl.when(jnp.logical_not(own))
            def _():
                bytes_of(buf, sem)()

        return wait

    def cols(at, size):
        return pl.ds(pl.multiple_of(at, 128), size)

    krow = cols(core * 128, 128)
    mine = cols((4 * yy + xx) * PIECE, PIECE)
    owned = cols((4 * j + xx) * PIECE, PIECE)
    block = cols(xx * PIECE, PIECE)

    local("hid", r.hidden_in, r.hid_v)

    barrier = pltpu.get_barrier_semaphore()

    def greet(d, z):
        @pl.when(jnp.logical_not((d == i) & (z == j)))
        def _():
            pl.semaphore_signal(barrier, inc=1, device_id=(d, z), device_id_type=MESH)

    def greet_far(k, _):
        greet(2 * k + core, yy)
        greet(8 * yy + 2 * lax.rem(k, 4) + core, lax.div(k, 4))
        return 0

    def greet_plane(k, _):
        greet(k, j)
        return 0

    lax.fori_loop(0, CHIPS, greet_far, 0)
    lax.fori_loop(0, NDP, greet_plane, 0)

    local("rg", r.rec_gain.at[:, mine], r.rgain_v.at[0])
    local("rg1", r.rec_gain.at[:, owned], r.rgain_v.at[1])
    merged = []
    for l in range(LAYERS):
        for q in range(2):
            merged.append((("in", l), r.rec_in_x.at[l], r.wi.at[l], q, 2 * q * PIECE, PIECE))
            merged.append((("in", l), r.rec_in_y.at[l], r.wi.at[l], q, (2 * q + 1) * PIECE, PIECE))
        merged.append((("out", l), r.rec_out.at[l], r.wr.at[l], 0, 0, HALF))
    merged.append((("q",), r.attn_q, r.wq, 0, 0, HALF))
    merged.append((("o",), r.attn_out, r.wo, 0, 0, HALF))

    def weight_part(src, q, size, c):
        return src.at[:, cols(c * HALF + q * size, size)]

    for n, (tag, src, dst, q, at, size) in enumerate(merged):
        local(("own", *tag, n), weight_part(src, q, size, core), dst.at[krow, pl.ds(at, size)])
    local("cw", r.conv_weight.at[:, :, block], r.cw_v)
    local("cb", r.conv_bias.at[:, block], r.cb_v)
    local("gxb", r.gate_x_bias.at[:, block], r.gxb_v)
    local("gab", r.gate_a_bias.at[:, block], r.gab_v)
    local("dec", r.decay_param.at[:, block], r.dec_v)
    local("gxw", r.gate_x_weight.at[:, xx], r.gxw_v)
    local("gaw", r.gate_a_weight.at[:, xx], r.gaw_v)
    local("sc", r.scale_index, r.scale_s)
    local("pos", r.positions, r.pos_s)
    local("win", r.conv_state, r.win_v)
    local("ag", r.attn_gain.at[:, owned], r.again_v)
    local("wkv", r.attn_kv, r.wkv_v)
    local("key", r.key_cache, r.key_v)
    local("val", r.value_cache, r.val_v)

    late3 = lax.broadcasted_iota(jnp.int32, (NX, ROWS, PIECE), 1) >= SEQ

    def turned(values):
        return pltpu.roll(values, SEQ, 1)

    lane = lax.broadcasted_iota(jnp.int32, (BLOCK, 128), 1)
    diag = lane == lax.broadcasted_iota(jnp.int32, (BLOCK, 128), 0)

    def norm_line(k, line):
        me = NX * j + xx
        r.nsend[k] = line
        r.nbuf[k, me] = line
        pair = sems()

        def one(n, _):
            x, z = lax.div(n, NMP), lax.rem(n, NMP)

            @pl.when(jnp.logical_not((x == xx) & (z == j)))
            def _():
                remote(r.nsend.at[k], r.nbuf.at[k, me], pair, (8 * yy + 2 * x + core, z))

            return 0

        lax.fori_loop(0, CHIPS, one, 0)
        view = r.nbuf.at[k, pl.ds(0, CHIPS - 1)]
        pending["norm", k] = bytes_of(view, pair[1])
        pending["norm sent", k] = bytes_of(view, pair[0])

    def norm_first():
        h = r.h_v[...]
        sq = jnp.broadcast_to(jnp.sum(h * h, axis=-1, keepdims=True), (ROWS, 128))
        here = lax.broadcasted_iota(jnp.int32, (ROWS, 128), 1) - 8 * xx
        at = here == lax.broadcasted_iota(jnp.int32, (ROWS, 128), 0)
        line = jnp.sum(jnp.where(at, sq, 0.0), axis=0, keepdims=True)
        norm_line(0, line)

    def norm_send(k):
        x = r.x_v[...]
        sq = jnp.sum((x * x).reshape(BLOCK, PIECE), axis=-1, keepdims=True)
        norm_line(k, jnp.sum(jnp.where(diag, jnp.broadcast_to(sq, (BLOCK, 128)), 0.0), axis=0, keepdims=True))

    def norm_scale(k):
        take(("norm", k))
        total = r.nbuf[k, 0]
        for n in range(1, CHIPS):
            total = total + r.nbuf[k, n]
        line = lax.rsqrt(total * (1.0 / 4096.0) + 1e-06)
        return jnp.sum(jnp.where(diag, jnp.broadcast_to(line, (BLOCK, 128)), 0.0), axis=-1, keepdims=True)

    def half_sent(name, half, pair):
        pending[name] = all_but_self(half, pair[1], diagonal)
        pending[name + " sent"] = all_but_self(half, pair[0], diagonal)

    def spread(k):
        pair = sems()
        me = lax.div(i, 2)

        def one(n, _):
            q = lax.div(n, NMP)
            z = lax.rem(n, NMP)
            d = 8 * j + 2 * q + core

            @pl.when(jnp.logical_not((d == i) & (z == j)))
            def _():
                remote(r.pieces.at[k, q], r.spread_b.at[k, core, me], pair, (d, z))

            return 0

        lax.fori_loop(0, CHIPS, one, 0)
        half_sent(f"spread{k}", r.spread_b.at[k, core], pair)

        @pl.when(diagonal)
        def _():
            r.spread_b[k, core, me] = r.pieces[k, xx]

    def gather(k):
        pair = sems()

        def one(z, _):
            d = 8 * j + 2 * xx + core

            @pl.when(jnp.logical_not((d == i) & (z == j)))
            def _():
                remote(r.act_s.at[k], r.act_b.at[k, core, yy], pair, (d, z))

            return 0

        lax.fori_loop(0, NMP, one, 0)
        half_sent(f"gather{k}", r.act_b.at[k, core], pair)

        @pl.when(diagonal)
        def _():
            r.act_b[k, core, yy] = r.act_s[k]

    def halves(name, buf):
        own = buf.at[core]
        take(name)
        pair = sems()
        remote(own, own, pair, (mate, j))
        pending[name + " on"] = bytes_of(own, pair[0])
        yield core, own
        bytes_of(own, pair[1])()
        yield 1 - core, buf.at[1 - core]

    def gathered(k):
        for c, part in halves(f"gather{k}", r.act_b.at[k]):
            yield c, part[...].reshape(4 * BLOCK, PIECE)

    def spread_in(k, gain):
        for c, part in halves(f"spread{k}", r.spread_b.at[k]):
            act = part[...].astype(F32).reshape(4 * BLOCK, PIECE)
            yield c, (act if gain is None else act * gain).astype(BF16)

    def reduce_start(name, buf):
        pair = sems()
        pending[name] = all_but_self(buf, pair[1], inside)
        pending[name + " sent"] = all_but_self(buf, pair[0], inside)
        return pair

    def reduce(pair, send, buf, c):
        me = NX * yy + xx

        def one(n, _):
            q, at = lax.div(n, 4), lax.rem(n + yy + 2, 4)
            d = 8 * at + 2 * (2 * core + q) + c

            @pl.when(d != i)
            def _():
                remote(send.at[q, 4 * c + at], buf.at[me], pair, (d, j))

            return 0

        lax.fori_loop(0, BLOCKS, one, 0)

    def reduce_own(send, buf):
        @pl.when(inside)
        def _():
            buf[NX * yy + xx] = send[xx - 2 * core, 4 * core + yy]

    def total_of(buf, at):
        acc = buf[0, :, at].astype(F32)
        for n in range(1, CHIPS):
            acc = acc + buf[n, :, at].astype(F32)
        return acc

    def reduce_all_start(name, buf):
        pair = sems()
        view = buf.at[pl.ds(0, NDP - 1)]
        pending[name] = bytes_of(view, pair[1])
        pending[name + " sent"] = bytes_of(view, pair[0])
        return pair

    def reduce_all(pair, send, buf, c):
        def one(n, _):
            d = 2 * lax.rem(lax.div(i, 2) + 8 + n, CHIPS) + c

            @pl.when(d != i)
            def _():
                remote(send.at[row_slot(d)], buf.at[i], pair, (d, j))

            return 0

        lax.fori_loop(0, CHIPS, one, 0)

    def reduce_all_own(send, buf):
        buf[i] = send[row_slot(i)]

    def summed(buf, c, at):
        acc = buf[c, :, at].astype(F32)
        for p in range(1, NDP // 2):
            acc = acc + buf[2 * p + c, :, at].astype(F32)
        return acc

    def row_slot(d):
        return CHIPS * lax.rem(d, 2) + lax.div(d, 2)

    take("hid")
    r.h_v[0:SEQ, :] = r.hid_v[0].astype(F32)
    r.h_v[SEQ:ROWS, :] = r.hid_v[1].astype(F32)
    for q in range(NMP):
        r.pieces[0, q] = r.h_v[:, q * PIECE : (q + 1) * PIECE].astype(BF16)

    met = 2 * CHIPS - 1 + NDP - 1
    pl.semaphore_wait(barrier, jnp.where(diagonal, met - 1, met))
    spread(0)

    def trade(tag):
        pair = sems()
        total = 0
        for t, src, dst, q, at, size in merged:
            if t == tag:
                remote(weight_part(src, q, size, 1 - core), dst.at[krow, pl.ds(at, size)], pair, (mate, j))
                total += size
        for t, src, dst, q, at, size in merged:
            if t == tag:
                whole = dst.at[krow, pl.ds(0, total)]
        pending["mate", *tag] = bytes_of(whole, pair[1])
        pending["mate sent", *tag] = bytes_of(whole, pair[0])

    def merged_ready(tag):
        for n, (t, *_) in enumerate(merged):
            if t == tag:
                take(("own", *tag, n))
        take(("mate", *tag))

    def states_send():
        pairs = sems(), sems(), sems()

        def one(n, _):
            x = lax.rem(xx + n, NX)
            device = (8 * yy + 2 * x + core, j)
            remote(r.pieces.at[0, x], r.ent_b.at[xx], pairs[2], device)
            remote(r.lru_state.at[:, :, cols(x * PIECE, PIECE)], r.lru_b.at[xx], pairs[0], device)
            remote(r.conv_state.at[:, :, :, cols(x * PIECE, PIECE)], r.win_b.at[xx], pairs[1], device)
            return 0

        lax.fori_loop(1, NX, one, 0)
        local("lru own", r.lru_state.at[:, :, block], r.lru_b.at[xx])
        local("win own", r.conv_state.at[:, :, :, block], r.win_b.at[xx])
        r.ent_b[xx] = r.pieces[0, xx]
        for name, buf, pair in (
            ("lru", r.lru_b, pairs[0]),
            ("window", r.win_b, pairs[1]),
            ("entering", r.ent_b, pairs[2]),
        ):
            view = buf.at[pl.ds(0, NX - 1)]
            pending[name] = bytes_of(view, pair[1])
            pending[name + " sent"] = bytes_of(view, pair[0])

    trade(("in", 0))
    norm_first()
    states_send()
    trade(("out", 0))
    trade(("in", 1))
    trade(("out", 1))
    trade(("q",))
    trade(("o",))

    scales = []

    def prepare():
        take("pos")
        srow = lax.broadcasted_iota(jnp.int32, (ROWS, SLOTS), 0)
        slot = lax.broadcasted_iota(jnp.int32, (ROWS, SLOTS), 1) + j * SLOTS
        seq = srow & 3
        pos = jnp.where(
            seq == 0,
            r.pos_s[0],
            jnp.where(seq == 1, r.pos_s[1], jnp.where(seq == 2, r.pos_s[2], r.pos_s[3])),
        )
        step = lax.shift_right_logical(srow, 2)
        held = pos - 1 - ((pos - 1 - slot) & (WIN - 1))
        r.mask_v[...] = jnp.where((held >= 0) & (held >= pos + step - (WIN - 1)), 1.0, 0.0).astype(F32)
        take("win")
        for l in range(LAYERS):
            r.conv_out[l, 0] = r.win_v[l, 2]
        take("sc", "lru", "lru own", "window", "win own")
        for l in range(LAYERS):
            power = (r.scale_s[l].astype(F32) - 4.0) * 0.5
            scales.append(jnp.exp2(jnp.full((1, 128), power, F32))[:, :1])
            for x in range(NX):
                r.st_v[l, x, 0:SEQ, :] = r.lru_b[x, l].astype(F32) * scales[l]
                r.st_v[l, x, SEQ:ROWS, :] = jnp.zeros((SEQ, PIECE), F32)
                w0 = r.win_b[x, l, 0].astype(F32)
                w1 = r.win_b[x, l, 1].astype(F32)
                w2 = r.win_b[x, l, 2].astype(F32)
                r.t0_v[l, x, 0:SEQ, :] = w0
                r.t0_v[l, x, SEQ:ROWS, :] = w1
                r.t1_v[l, x, 0:SEQ, :] = w1
                r.t1_v[l, x, SEQ:ROWS, :] = w2
                r.t2_v[l, x, 0:SEQ, :] = w2
                r.t2_v[l, x, SEQ:ROWS, :] = jnp.zeros((SEQ, PIECE), F32)
        take("cw", "cb", "gxb", "gab", "dec", "gxw", "gaw", "rg1", "entering")
        r.x_v[...] = r.ent_b[...].astype(F32)

    def give_back(l):
        pairs = sems(), sems()

        def one(n, _):
            x = lax.rem(xx + n, NX)
            device = (8 * yy + 2 * x + core, j)
            remote(r.lru_s.at[l, x], r.lru_out.at[l, :, block], pairs[0], device)
            remote(r.win_s.at[l, x], r.conv_out.at[l, pl.ds(1, 2), :, block], pairs[1], device)
            return 0

        lax.fori_loop(1, NX, one, 0)
        r.lru_out[l, :, block] = r.lru_s[l, xx]
        r.conv_out[l, 1:3, :, block] = r.win_s[l, xx]
        for name, buf, pair in (("lru", r.lru_s, pairs[0]), ("window", r.win_s, pairs[1])):
            view = buf.at[l, pl.ds(0, NX - 1)]
            pending[name + " back", l] = bytes_of(view, pair[1])
            pending[name + " back sent", l] = bytes_of(view, pair[0])

    def recurrent(l, parts, meanwhile):
        pair = reduce_start(f"in{l}", r.in_b.at[l])
        for c, act in parts:
            for n in range(4):
                part = jnp.dot(act, r.wi[l, :, n * PIECE : (n + 1) * PIECE], preferred_element_type=F32)
                at = slice((n % 2) * PIECE, (n % 2 + 1) * PIECE)
                r.in_s[l, n // 2, pl.ds(4 * c, 4), :, at] = part.reshape(4, BLOCK, PIECE).astype(BF16)
            reduce(pair, r.in_s.at[l], r.in_b.at[l], c)
        reduce_own(r.in_s.at[l], r.in_b.at[l])
        meanwhile()
        decay = r.dec_v[l : l + 1, :]
        soft = jnp.maximum(decay, 0.0) + jnp.log1p(jnp.exp(-jnp.abs(decay)))
        soft = soft.reshape(1, 1, PIECE)

        def tap(n):
            return r.cw_v[l, n : n + 1, :].reshape(1, 1, PIECE)

        bias = r.cb_v[l : l + 1, :].reshape(1, 1, PIECE)
        early = tap(0) * r.t0_v[l] + tap(1) * r.t1_v[l] + bias
        scale = norm_scale(l)
        take(f"in{l}")
        u = (total_of(r.in_b.at[l], slice(0, PIECE)) * scale).astype(BF16).astype(F32)
        u = u.reshape(NX, ROWS, PIECE)
        v = (total_of(r.in_b.at[l], slice(PIECE, HALF)) * scale).reshape(NX, ROWS, PIECE)
        u_turned = turned(u)
        t2 = jnp.where(late3, u_turned, r.t2_v[l])
        filtered = early + tap(2) * t2 + tap(3) * u
        half = filtered.reshape(BLOCK, PIECE).astype(BF16)
        gx = jnp.dot(half, r.gxw_v[l], preferred_element_type=F32) + r.gxb_v[l : l + 1, :]
        ga = jnp.dot(half, r.gaw_v[l], preferred_element_type=F32) + r.gab_v[l : l + 1, :]
        gx = (1.0 / (1.0 + jnp.exp(-gx))).reshape(NX, ROWS, PIECE)
        ga = (1.0 / (1.0 + jnp.exp(-ga))).reshape(NX, ROWS, PIECE)
        log_a = -8.0 * ga * soft
        a = jnp.exp(log_a)
        add = jnp.sqrt(1.0 - jnp.exp(2.0 * log_a)) * (gx * filtered)
        first = a * r.st_v[l] + add
        second = a * turned(first) + add
        state = jnp.where(late3, second, first)
        gelu = 0.5 * v * (1.0 + jnp.tanh(0.7978845608028654 * (v + 0.044715 * (v * v * v))))
        r.act_s[2 * l] = (state * gelu).reshape(BLOCK, PIECE).astype(BF16)
        gather(2 * l)
        state_turned = turned(state)
        for x in range(NX):
            r.lru_s[l, x] = (state_turned[x, 0:SEQ] / scales[l]).astype(BF16)
            r.win_s[l, x, 0] = u[x, 0:SEQ].astype(BF16)
            r.win_s[l, x, 1] = u_turned[x, 0:SEQ].astype(BF16)
        give_back(l)

        merged_ready(("out", l))
        pair = reduce_start(f"out{l}", r.out_b.at[l])
        for c, act in gathered(2 * l):
            for n in range(2):
                part = jnp.dot(act, r.wr[l, :, n * PIECE : (n + 1) * PIECE], preferred_element_type=F32)
                r.out_s[l, n, pl.ds(4 * c, 4)] = part.reshape(4, BLOCK, PIECE).astype(BF16)
            reduce(pair, r.out_s.at[l], r.out_b.at[l], c)
        reduce_own(r.out_s.at[l], r.out_b.at[l])
        take(f"out{l}")
        r.x_v[...] = r.x_v[...] + total_of(r.out_b.at[l], slice(0, PIECE)).reshape(NX, ROWS, PIECE)

    def next_act(k, gain):
        r.act_s[k] = (r.x_v[...].reshape(BLOCK, PIECE) * gain).astype(BF16)
        gather(k)

    merged_ready(("in", 0))
    take("rg")
    recurrent(0, spread_in(0, r.rgain_v[0, 0:1, :]), prepare)
    next_act(1, r.rgain_v[1, 1:2, :])
    norm_send(1)
    merged_ready(("in", 1))
    recurrent(1, gathered(1), lambda: None)
    take("ag")
    next_act(3, r.again_v[...])
    norm_send(2)

    pair = sems()
    r.res_s[...] = r.x_v[...]

    def stream_send(n, _):
        x = lax.rem(xx + n, NX)
        remote(r.res_s.at[x], r.res_b.at[xx], pair, (8 * yy + 2 * x + core, j))
        return 0

    lax.fori_loop(1, NX, stream_send, 0)
    r.res_b[xx] = r.res_s[xx]
    view = r.res_b.at[pl.ds(0, NX - 1)]
    pending["stream"] = bytes_of(view, pair[1])
    pending["stream sent"] = bytes_of(view, pair[0])

    take("wkv", "key", "val")
    merged_ready(("q",))
    pair = reduce_all_start("q", r.q_b)
    for c, act in gathered(3):
        rows = pl.ds(CHIPS * c, CHIPS)
        for n in range(2):
            at = slice(n * PIECE, (n + 1) * PIECE)
            part = jnp.dot(act, r.wq[:, at], preferred_element_type=F32)
            r.q_s[rows, :, at] = part.reshape(CHIPS, ROWS, PIECE).astype(BF16)
        act = r.act_b[3, c, :, :, krow].reshape(4 * BLOCK, 128)
        part = jnp.dot(act, r.wkv_v[...], preferred_element_type=F32)
        r.q_s[rows, :, HALF:] = part.reshape(CHIPS, ROWS, 128).astype(BF16)
        reduce_all(pair, r.q_s, r.q_b, c)
    reduce_all_own(r.q_s, r.q_b)
    scale = norm_scale(2)
    own = jnp.zeros((ROWS, 1), F32)
    for x in range(NX):
        own = jnp.where(xx == x, scale[x * ROWS : (x + 1) * ROWS], own)
    scale = own
    take("q")
    for c in range(2):
        at = slice(c * HALF, (c + 1) * HALF)
        r.zsend[:, at] = (summed(r.q_b, c, slice(0, HALF)) * scale).astype(BF16)
    at = slice(HALF, HALF + 128)
    kv = (summed(r.q_b, 0, at) + summed(r.q_b, 1, at)) * scale
    r.zsend[:, FEAT:] = kv.astype(BF16)
    query_pair, part_pair, top_pair = sems(), sems(), sems()

    def query_send(d, _):
        remote(r.zsend, r.zbuf.at[j], query_pair, (i, lax.rem(j + d, NMP)))
        return 0

    lax.fori_loop(1, NMP, query_send, 0)
    view = r.zbuf.at[pl.ds(0, NMP - 1)]
    pending["query"] = bytes_of(view, query_pair[1])
    pending["query sent"] = bytes_of(view, query_pair[0])
    r.zbuf[j] = r.zsend[...]
    r.new_kv[0] = kv[0:SEQ].astype(BF16)
    r.new_kv[1] = pltpu.roll(kv, SEQ, 0)[0:SEQ].astype(BF16)
    take("query")

    rows = HEADS * ROWS
    query = jnp.concatenate(
        [
            r.zbuf[z, :, h * HEAD_DIM : (h + 1) * HEAD_DIM].astype(F32)
            for z in range(NMP)
            for h in range(HEADS // NMP)
        ],
        axis=0,
    ).astype(BF16)
    which = lax.broadcasted_iota(jnp.int32, (rows, SLOTS), 0) & 3
    scores = None
    for b in range(SEQ):
        one = lax.dot_general(
            query, r.key_v[b], (((1,), (1,)), ((), ())), preferred_element_type=F32
        )
        scores = one if scores is None else jnp.where(which == b, one, scores)
    mask = jnp.broadcast_to(r.mask_v[...][None], (HEADS, ROWS, SLOTS)).reshape(rows, SLOTS)
    scores = jnp.where(mask > 0.5, scores * HEAD_DIM ** (-0.5), -1e30)
    top = jnp.max(scores, axis=-1, keepdims=True)
    weight = jnp.exp(scores - top) * mask
    total = jnp.sum(weight, axis=-1, keepdims=True)
    values = None
    for b in range(SEQ):
        one = jnp.dot(
            jnp.where(which == b, weight, 0.0).astype(BF16), r.val_v[b], preferred_element_type=F32
        )
        values = one if values is None else values + one
    lane = lax.broadcasted_iota(jnp.int32, (rows, 128), 1)
    r.csend[...] = values.reshape(HEADS, ROWS, HEAD_DIM).astype(BF16)
    r.tsend[...] = jnp.where(lane < 64, top, total).reshape(HEADS, ROWS, 128)

    def part_send(d, _):
        z = lax.rem(j + d, NMP)
        group = pl.ds(4 * z, 4)
        remote(r.csend.at[group], r.cbuf.at[j], part_pair, (i, z))
        remote(r.tsend.at[group], r.tbuf.at[j], top_pair, (i, z))
        return 0

    lax.fori_loop(1, NMP, part_send, 0)
    for name, buf, pair in (("part", r.cbuf, part_pair), ("top", r.tbuf, top_pair)):
        view = buf.at[pl.ds(0, NMP - 1)]
        pending[name] = bytes_of(view, pair[1])
        pending[name + " sent"] = bytes_of(view, pair[0])
    r.cbuf[j] = r.csend[pl.ds(4 * j, 4)]
    r.tbuf[j] = r.tsend[pl.ds(4 * j, 4)]

    lateh = lax.broadcasted_iota(jnp.int32, (ROWS, HEAD_DIM), 0) >= SEQ
    late1 = lax.broadcasted_iota(jnp.int32, (ROWS, 1), 0) >= SEQ

    def pair(lo, hi):
        at = slice(FEAT, FEAT + 128)
        both = jnp.concatenate([r.zbuf[lo, :, at].astype(F32), r.zbuf[hi, :, at].astype(F32)], axis=1)
        turned = pltpu.roll(both, SEQ, 0)
        return jnp.where(lateh, turned, both), jnp.where(lateh, both, turned)

    key0, key1 = pair(0, 1)
    val0, val1 = pair(2, 3)
    fresh = []
    for h in range(4):
        head = r.zsend[:, h * HEAD_DIM : (h + 1) * HEAD_DIM].astype(F32)
        s0 = jnp.sum(head * key0, axis=-1, keepdims=True) * HEAD_DIM ** (-0.5)
        s1 = jnp.sum(head * key1, axis=-1, keepdims=True) * HEAD_DIM ** (-0.5)
        fresh.append((s0, jnp.where(late1, s1, -1e30)))
    take("part", "top")
    for h in range(4):
        s0, s1 = fresh[h]
        tops = [r.tbuf[z, h, :, 0:1] for z in range(NMP)]
        best = jnp.maximum(s0, s1)
        for t in tops:
            best = jnp.maximum(best, t)
        w0 = jnp.exp(s0 - best)
        w1 = jnp.where(late1, jnp.exp(s1 - best), 0.0)
        den = w0 + w1
        num = w0.astype(BF16).astype(F32) * val0 + w1.astype(BF16).astype(F32) * val1
        for z in range(NMP):
            fade = jnp.exp(tops[z] - best)
            den = den + fade * r.tbuf[z, h, :, 64:65]
            num = num + fade * r.cbuf[z, h].astype(F32)
        r.pieces[1, h] = (num / den).astype(BF16)
    spread(1)
    merged_ready(("o",))
    pair = reduce_all_start("o", r.o_b)
    for c, act in spread_in(1, None):
        for n in range(2):
            at = slice(n * PIECE, (n + 1) * PIECE)
            part = jnp.dot(act, r.wo[:, at], preferred_element_type=F32)
            r.o_s[pl.ds(CHIPS * c, CHIPS), :, at] = part.reshape(CHIPS, ROWS, PIECE).astype(BF16)
        reduce_all(pair, r.o_s, r.o_b, c)
    reduce_all_own(r.o_s, r.o_b)
    take("stream", "o")
    for q in range(NMP):
        at = slice((q % 2) * PIECE, (q % 2 + 1) * PIECE)
        x = r.res_b[q] + summed(r.o_b, q // 2, at)
        at = slice(q * PIECE, (q + 1) * PIECE)
        r.hidden_out[0, :, at] = x[0:SEQ].astype(BF16)
        r.hidden_out[1, :, at] = pltpu.roll(x, SEQ, 0)[0:SEQ].astype(BF16)

    take(*list(pending))


def hand_over(*refs):
    for src, dst in zip(refs[:4], refs[4:]):
        dst[...] = src[...]


def body(*args):
    args = list(args)
    args[15] = args[15].reshape(1, -1)
    shape = jax.ShapeDtypeStruct
    hbm = pl.BlockSpec(memory_space=pltpu.HBM)
    vmem = pl.BlockSpec(memory_space=pltpu.VMEM)
    outs = pl.pallas_call(
        kernel,
        out_shape=(
            shape((STEPS, SEQ, FEAT), BF16),
            shape((LAYERS, SEQ, FEAT), BF16),
            shape((LAYERS, 3, SEQ, FEAT), BF16),
            shape((STEPS, SEQ, 128), BF16),
        ),
        in_specs=[hbm] * 22,
        out_specs=(vmem,) * 4,
        scratch_shapes=[kind for _, kind in scratch_list()],
        compiler_params=pltpu.CompilerParams(
            collective_id=0, has_side_effects=True, vmem_limit_bytes=VMEM
        ),
    )(*args)
    return pl.pallas_call(
        hand_over,
        out_shape=tuple(shape(out.shape, out.dtype) for out in outs),
        in_specs=[vmem] * 4,
        out_specs=(vmem,) * 4,
    )(*outs)


def solution(mesh):
    placed = (
        P(None, "dp", "mp"),
        P(),
        P(None, "dp", "mp"),
        P(None, "dp", "mp"),
        P(None, None, "mp"),
        P(None, "mp"),
        P(None, "mp", None, None),
        P(None, "mp"),
        P(None, "mp", None, None),
        P(None, "mp"),
        P(None, "mp"),
        P(None, "dp", "mp"),
        P(None, "dp", "mp"),
        P(None, None, "dp", "mp"),
        P(),
        P(),
        P("dp", "mp"),
        P("dp", "mp"),
        P("dp", "mp"),
        P("dp", "mp", None),
        P("dp", "mp", None),
        P("dp"),
    )
    return jax.shard_map(
        body,
        mesh=mesh,
        in_specs=placed,
        out_specs=(
            P(None, "dp", "mp"),
            P(None, "dp", "mp"),
            P(None, None, "dp", "mp"),
            P(None, "dp", "mp"),
        ),
        check_vma=False,
    )
```

```python
import jax
import jax.numpy as jnp
from jax import lax
from jax.experimental import pallas as pl
from jax.experimental.pallas import tpu as pltpu
from jax.sharding import PartitionSpec as P

HEADS = 16
HEAD_DIM = 256
WIN = 2048
LAYERS = 2
STEPS = 2
F32 = jnp.float32
BF16 = jnp.bfloat16
MESH = pl.DeviceIdType.MESH

NDP = 32
NMP = 4
NX = 4
ROWS = 8
SEQ = 4
FEAT = 1024
PIECE = 256
HALF = 512
SLOTS = 512
BLOCKS = 8
BLOCK = 32
CHIPS = 16
VMEM = 67043328


def scratch_list():
    V = pltpu.VMEM
    DMA = pltpu.SemaphoreType.DMA
    return [
        ("hid_v", V((STEPS, SEQ, FEAT), BF16)),
        ("rgain_v", V((2, LAYERS, PIECE), F32)),
        ("again_v", V((1, PIECE), F32)),
        ("cw_v", V((LAYERS, 4, PIECE), F32)),
        ("cb_v", V((LAYERS, PIECE), F32)),
        ("gxw_v", V((LAYERS, PIECE, PIECE), BF16)),
        ("gxb_v", V((LAYERS, PIECE), F32)),
        ("gaw_v", V((LAYERS, PIECE, PIECE), BF16)),
        ("gab_v", V((LAYERS, PIECE), F32)),
        ("dec_v", V((LAYERS, PIECE), F32)),
        ("win_v", V((LAYERS, 3, SEQ, FEAT), BF16)),
        ("key_v", V((SEQ, SLOTS, HEAD_DIM), BF16)),
        ("val_v", V((SEQ, SLOTS, HEAD_DIM), BF16)),
        ("wkv", V((PIECE, 128), BF16)),
        ("wi", V((LAYERS, PIECE, 2 * FEAT), BF16)),
        ("wr", V((LAYERS, PIECE, FEAT), BF16)),
        ("wq", V((PIECE, FEAT), BF16)),
        ("wo", V((PIECE, FEAT), BF16)),
        ("scale_s", pltpu.SMEM((LAYERS,), jnp.int32)),
        ("pos_s", pltpu.SMEM((SEQ,), jnp.int32)),
        ("x_v", V((NX, ROWS, PIECE), F32)),
        ("h_v", V((ROWS, FEAT), F32)),
        ("st_v", V((LAYERS, NX, ROWS, PIECE), F32)),
        ("t0_v", V((LAYERS, NX, ROWS, PIECE), F32)),
        ("t1_v", V((LAYERS, NX, ROWS, PIECE), F32)),
        ("t2_v", V((LAYERS, NX, ROWS, PIECE), F32)),
        ("mask_v", V((ROWS, SLOTS), F32)),
        ("lru_b", V((NX, LAYERS, SEQ, PIECE), BF16)),
        ("win_b", V((NX, LAYERS, 3, SEQ, PIECE), BF16)),
        ("lru_s", V((LAYERS, NX, SEQ, PIECE), BF16)),
        ("win_s", V((LAYERS, NX, 2, SEQ, PIECE), BF16)),
        ("pieces", V((2, NMP, ROWS, PIECE), BF16)),
        ("spread_b", V((2, CHIPS, ROWS, PIECE), BF16)),
        ("act_s", V((4, BLOCK, PIECE), BF16)),
        ("act_b", V((4, 4, BLOCK, PIECE), BF16)),
        ("in_s", V((LAYERS, NX, 4, BLOCK, HALF), BF16)),
        ("in_b", V((LAYERS, CHIPS, BLOCK, HALF), BF16)),
        ("out_s", V((LAYERS, NX, 4, BLOCK, PIECE), BF16)),
        ("out_b", V((LAYERS, CHIPS, BLOCK, PIECE), BF16)),
        ("q_s", V((CHIPS, ROWS, FEAT + 128), BF16)),
        ("q_b", V((CHIPS, ROWS, FEAT + 128), BF16)),
        ("o_s", V((CHIPS, ROWS, FEAT), BF16)),
        ("o_b", V((CHIPS, ROWS, FEAT), BF16)),
        ("ent_b", V((NX, ROWS, PIECE), BF16)),
        ("res_s", V((NX, ROWS, PIECE), F32)),
        ("res_b", V((NX, ROWS, PIECE), F32)),
        ("nsend", V((3, 1, 128), F32)),
        ("nbuf", V((3, CHIPS, 1, 128), F32)),
        ("zsend", V((ROWS, FEAT + 128), BF16)),
        ("zbuf", V((NMP, ROWS, FEAT + 128), BF16)),
        ("csend", V((HEADS, ROWS, HEAD_DIM), BF16)),
        ("cbuf", V((NMP, 4, ROWS, HEAD_DIM), BF16)),
        ("tsend", V((HEADS, ROWS, 128), F32)),
        ("tbuf", V((NMP, 4, ROWS, 128), F32)),
        ("lsem", DMA((32,))),
        ("snd", DMA((48,))),
        ("rcv", DMA((48,))),
    ]


NAMES = (
    "hidden_in",
    "rec_gain",
    "rec_in_x",
    "rec_in_y",
    "conv_weight",
    "conv_bias",
    "gate_x_weight",
    "gate_x_bias",
    "gate_a_weight",
    "gate_a_bias",
    "decay_param",
    "rec_out",
    "lru_state",
    "conv_state",
    "scale_index",
    "attn_gain",
    "attn_q",
    "attn_kv",
    "attn_out",
    "key_cache",
    "value_cache",
    "positions",
    "hidden_out",
    "lru_out",
    "conv_out",
    "new_kv",
)


class Refs:
    def __init__(self, refs):
        names = (*NAMES, *(name for name, _ in scratch_list()))
        for name, ref in zip(names, refs, strict=True):
            setattr(self, name, ref)


def kernel(*refs):
    r = Refs(refs)
    i = lax.axis_index("dp")
    j = lax.axis_index("mp")
    core = lax.rem(i, 2)
    mate = i + 1 - 2 * core
    yy = lax.div(i, 8)
    xx = lax.div(lax.rem(i, 8), 2)
    diagonal = yy == j
    place = lax.div(i, 2)

    pending = {}
    used = [0, 0]

    def take(*names):
        for name in names:
            pending.pop(name)()

    def sems():
        used[1] += 1
        assert used[1] <= 48
        return r.snd.at[used[1] - 1], r.rcv.at[used[1] - 1]

    def local(name, src, dst):
        sem = r.lsem.at[used[0]]
        used[0] += 1
        copy = pltpu.make_async_copy(src, dst, sem)
        copy.start()
        pending[name] = copy.wait

    def remote(src, dst, pair, device):
        pltpu.make_async_remote_copy(
            src_ref=src,
            dst_ref=dst,
            send_sem=pair[0],
            recv_sem=pair[1],
            device_id=device,
            device_id_type=MESH,
        ).start()

    def bytes_of(view, sem):
        return lambda: pltpu.make_async_copy(view, view, sem).wait()

    def all_but_self(buf, sem, own):
        def wait():
            @pl.when(own)
            def _():
                bytes_of(buf.at[pl.ds(0, buf.shape[0] - 1)], sem)()

            @pl.when(jnp.logical_not(own))
            def _():
                bytes_of(buf, sem)()

        return wait

    def cols(at, size):
        return pl.ds(pl.multiple_of(at, 128), size)

    krow = cols(core * 128, 128)
    mine = cols((4 * yy + xx) * PIECE, PIECE)
    owned = cols((4 * j + xx) * PIECE, PIECE)
    block = cols(xx * PIECE, PIECE)

    local("hid", r.hidden_in, r.hid_v)

    barrier = pltpu.get_barrier_semaphore()

    def greet(d, z):
        @pl.when(jnp.logical_not((d == i) & (z == j)))
        def _():
            pl.semaphore_signal(barrier, inc=1, device_id=(d, z), device_id_type=MESH)

    def greet_all(k, _):
        greet(2 * k + core, yy)
        greet(2 * k + core, j)
        greet(8 * yy + 2 * lax.rem(k, 4) + core, lax.div(k, 4))
        return 0

    lax.fori_loop(0, CHIPS, greet_all, 0)
    greet(mate, j)

    local("rg", r.rec_gain.at[:, mine], r.rgain_v.at[0])
    local("rg1", r.rec_gain.at[:, owned], r.rgain_v.at[1])
    merged = []
    for l in range(LAYERS):
        merged.append((("in", l), r.rec_in_x.at[l], r.wi.at[l, krow, pl.ds(0, FEAT)]))
        merged.append((("in", l), r.rec_in_y.at[l], r.wi.at[l, krow, pl.ds(FEAT, FEAT)]))
        merged.append((("out", l), r.rec_out.at[l], r.wr.at[l, krow, :]))
    merged.append((("q",), r.attn_q, r.wq.at[krow, :]))
    merged.append((("q",), r.attn_kv, r.wkv.at[krow, :]))
    merged.append((("o",), r.attn_out, r.wo.at[krow, :]))
    for n, (tag, src, dst) in enumerate(merged):
        local(("own", n), src, dst)
    local("cw", r.conv_weight.at[:, :, block], r.cw_v)
    local("cb", r.conv_bias.at[:, block], r.cb_v)
    local("gxb", r.gate_x_bias.at[:, block], r.gxb_v)
    local("gab", r.gate_a_bias.at[:, block], r.gab_v)
    local("dec", r.decay_param.at[:, block], r.dec_v)
    local("gxw", r.gate_x_weight.at[:, xx], r.gxw_v)
    local("gaw", r.gate_a_weight.at[:, xx], r.gaw_v)
    local("sc", r.scale_index, r.scale_s)
    local("pos", r.positions, r.pos_s)
    local("win", r.conv_state, r.win_v)
    local("ag", r.attn_gain.at[:, owned], r.again_v)
    local("key", r.key_cache, r.key_v)
    local("val", r.value_cache, r.val_v)

    late3 = lax.broadcasted_iota(jnp.int32, (NX, ROWS, PIECE), 1) >= SEQ

    def turned(values):
        return pltpu.roll(values, SEQ, 1)

    lane = lax.broadcasted_iota(jnp.int32, (BLOCK, 128), 1)
    diag = lane == lax.broadcasted_iota(jnp.int32, (BLOCK, 128), 0)

    def norm_line(k, line):
        me = NX * j + xx
        r.nsend[k] = line
        r.nbuf[k, me] = line
        pair = sems()

        def one(n, _):
            x, z = lax.div(n, NMP), lax.rem(n, NMP)

            @pl.when(jnp.logical_not((x == xx) & (z == j)))
            def _():
                remote(r.nsend.at[k], r.nbuf.at[k, me], pair, (8 * yy + 2 * x + core, z))

            return 0

        lax.fori_loop(0, CHIPS, one, 0)
        view = r.nbuf.at[k, pl.ds(0, CHIPS - 1)]
        pending["norm", k] = bytes_of(view, pair[1])
        pending["norm sent", k] = bytes_of(view, pair[0])

    def norm_first():
        h = r.h_v[...]
        sq = jnp.broadcast_to(jnp.sum(h * h, axis=-1, keepdims=True), (ROWS, 128))
        here = lax.broadcasted_iota(jnp.int32, (ROWS, 128), 1) - 8 * xx
        at = here == lax.broadcasted_iota(jnp.int32, (ROWS, 128), 0)
        line = jnp.sum(jnp.where(at, sq, 0.0), axis=0, keepdims=True)
        norm_line(0, line)

    def norm_send(k):
        x = r.x_v[...]
        sq = jnp.sum((x * x).reshape(BLOCK, PIECE), axis=-1, keepdims=True)
        norm_line(k, jnp.sum(jnp.where(diag, jnp.broadcast_to(sq, (BLOCK, 128)), 0.0), axis=0, keepdims=True))

    def norm_scale(k):
        take(("norm", k))
        total = r.nbuf[k, 0]
        for n in range(1, CHIPS):
            total = total + r.nbuf[k, n]
        line = lax.rsqrt(total * (1.0 / 4096.0) + 1e-06)
        return jnp.sum(jnp.where(diag, jnp.broadcast_to(line, (BLOCK, 128)), 0.0), axis=-1, keepdims=True)

    def spread(k):
        pair = sems()

        def one(n, _):
            q = lax.div(n, NMP)
            z = lax.rem(n + j + 2, NMP)
            d = 8 * j + 2 * q + core

            @pl.when(jnp.logical_not((d == i) & (z == j)))
            def _():
                remote(r.pieces.at[k, q], r.spread_b.at[k, place], pair, (d, z))

            return 0

        lax.fori_loop(0, CHIPS, one, 0)
        pending["spread", k] = all_but_self(r.spread_b.at[k], pair[1], diagonal)
        pending["spread sent", k] = all_but_self(r.spread_b.at[k], pair[0], diagonal)

        @pl.when(diagonal)
        def _():
            r.spread_b[k, place] = r.pieces[k, xx]

    def gather(k):
        pair = sems()

        def one(n, _):
            z = lax.rem(n + j + 2, NMP)
            d = 8 * j + 2 * xx + core

            @pl.when(jnp.logical_not((d == i) & (z == j)))
            def _():
                remote(r.act_s.at[k], r.act_b.at[k, yy], pair, (d, z))

            return 0

        lax.fori_loop(0, NMP, one, 0)
        pending["gather", k] = all_but_self(r.act_b.at[k], pair[1], diagonal)
        pending["gather sent", k] = all_but_self(r.act_b.at[k], pair[0], diagonal)

        @pl.when(diagonal)
        def _():
            r.act_b[k, yy] = r.act_s[k]

    def gathered(k):
        take(("gather", k))
        return r.act_b[k].reshape(4 * BLOCK, PIECE)

    def spread_in(k):
        take(("spread", k))
        return r.spread_b[k].astype(F32).reshape(4 * BLOCK, PIECE)

    def others(name, buf):
        pair = sems()
        view = buf.at[pl.ds(0, CHIPS - 1)]
        pending[name] = bytes_of(view, pair[1])
        pending[name + " sent"] = bytes_of(view, pair[0])
        return pair

    def column(n):
        return lax.rem(xx + (2, 1, 3, 0)[n], NX)

    def reduce(pair, send, buf, q):
        def one(n, _):
            at = lax.rem(n + yy + 2, 4)
            d = 8 * at + 2 * q + core

            @pl.when(d != i)
            def _():
                remote(send.at[q, at], buf.at[place], pair, (d, j))

            return 0

        lax.fori_loop(0, 4, one, 0)

    def reduce_all(pair, send, buf):
        def one(n, _):
            to = lax.rem(place + 8 + n, CHIPS)

            @pl.when(to != place)
            def _():
                remote(send.at[to], buf.at[place], pair, (2 * to + core, j))

            return 0

        lax.fori_loop(0, CHIPS, one, 0)
        buf[place] = send[place]

    def total_of(buf, at):
        acc = buf[0, :, at].astype(F32)
        for n in range(1, CHIPS):
            acc = acc + buf[n, :, at].astype(F32)
        return acc

    def summed(buf, at):
        acc = buf[0, :, at].astype(F32)
        for p in range(1, CHIPS):
            acc = acc + buf[p, :, at].astype(F32)
        return acc

    take("hid")
    r.h_v[0:SEQ, :] = r.hid_v[0].astype(F32)
    r.h_v[SEQ:ROWS, :] = r.hid_v[1].astype(F32)
    for q in range(NMP):
        r.pieces[0, q] = r.h_v[:, q * PIECE : (q + 1) * PIECE].astype(BF16)

    met = 3 * CHIPS - 1
    pl.semaphore_wait(barrier, jnp.where(diagonal, met - 1, met))
    spread(0)

    def trade():
        for n, (_, src, dst) in enumerate(merged):
            pair = sems()
            remote(src, dst, pair, (mate, j))
            pending["mate", n] = bytes_of(dst, pair[1])
            pending["mate sent", n] = bytes_of(dst, pair[0])

    def merged_ready(tag):
        for n, (t, *_) in enumerate(merged):
            if t == tag:
                take(("own", n), ("mate", n))

    def states_send():
        pairs = sems(), sems(), sems()

        def one(n, _):
            x = lax.rem(xx + n, NX)
            device = (8 * yy + 2 * x + core, j)
            remote(r.pieces.at[0, x], r.ent_b.at[xx], pairs[2], device)
            remote(r.lru_state.at[:, :, cols(x * PIECE, PIECE)], r.lru_b.at[xx], pairs[0], device)
            remote(r.conv_state.at[:, :, :, cols(x * PIECE, PIECE)], r.win_b.at[xx], pairs[1], device)
            return 0

        lax.fori_loop(1, NX, one, 0)
        local("lru own", r.lru_state.at[:, :, block], r.lru_b.at[xx])
        local("win own", r.conv_state.at[:, :, :, block], r.win_b.at[xx])
        r.ent_b[xx] = r.pieces[0, xx]
        for name, buf, pair in (
            ("lru", r.lru_b, pairs[0]),
            ("window", r.win_b, pairs[1]),
            ("entering", r.ent_b, pairs[2]),
        ):
            view = buf.at[pl.ds(0, NX - 1)]
            pending[name] = bytes_of(view, pair[1])
            pending[name + " sent"] = bytes_of(view, pair[0])

    trade()
    norm_first()
    states_send()

    scales = []

    def prepare():
        take("pos")
        srow = lax.broadcasted_iota(jnp.int32, (ROWS, SLOTS), 0)
        slot = lax.broadcasted_iota(jnp.int32, (ROWS, SLOTS), 1) + j * SLOTS
        seq = srow & 3
        pos = jnp.where(
            seq == 0,
            r.pos_s[0],
            jnp.where(seq == 1, r.pos_s[1], jnp.where(seq == 2, r.pos_s[2], r.pos_s[3])),
        )
        step = lax.shift_right_logical(srow, 2)
        held = pos - 1 - ((pos - 1 - slot) & (WIN - 1))
        r.mask_v[...] = jnp.where((held >= 0) & (held >= pos + step - (WIN - 1)), 1.0, 0.0).astype(F32)
        take("win")
        for l in range(LAYERS):
            r.conv_out[l, 0] = r.win_v[l, 2]
        take("sc", "lru", "lru own", "window", "win own")
        for l in range(LAYERS):
            power = (r.scale_s[l].astype(F32) - 4.0) * 0.5
            scales.append(jnp.exp2(jnp.full((1, 128), power, F32))[:, :1])
            for x in range(NX):
                r.st_v[l, x, 0:SEQ, :] = r.lru_b[x, l].astype(F32) * scales[l]
                r.st_v[l, x, SEQ:ROWS, :] = jnp.zeros((SEQ, PIECE), F32)
                w0 = r.win_b[x, l, 0].astype(F32)
                w1 = r.win_b[x, l, 1].astype(F32)
                w2 = r.win_b[x, l, 2].astype(F32)
                r.t0_v[l, x, 0:SEQ, :] = w0
                r.t0_v[l, x, SEQ:ROWS, :] = w1
                r.t1_v[l, x, 0:SEQ, :] = w1
                r.t1_v[l, x, SEQ:ROWS, :] = w2
                r.t2_v[l, x, 0:SEQ, :] = w2
                r.t2_v[l, x, SEQ:ROWS, :] = jnp.zeros((SEQ, PIECE), F32)
        take("cw", "cb", "gxb", "gab", "dec", "gxw", "gaw", "rg1", "entering")
        r.x_v[...] = r.ent_b[...].astype(F32)

    def give_back(l):
        pairs = sems(), sems()

        def one(n, _):
            x = lax.rem(xx + n, NX)
            device = (8 * yy + 2 * x + core, j)
            remote(r.lru_s.at[l, x], r.lru_out.at[l, :, block], pairs[0], device)
            remote(r.win_s.at[l, x], r.conv_out.at[l, pl.ds(1, 2), :, block], pairs[1], device)
            return 0

        lax.fori_loop(1, NX, one, 0)
        r.lru_out[l, :, block] = r.lru_s[l, xx]
        r.conv_out[l, 1:3, :, block] = r.win_s[l, xx]
        for name, buf, pair in (("lru", r.lru_s, pairs[0]), ("window", r.win_s, pairs[1])):
            view = buf.at[l, pl.ds(0, NX - 1)]
            pending[name + " back", l] = bytes_of(view, pair[1])
            pending[name + " back sent", l] = bytes_of(view, pair[0])

    def recurrent(l, act, meanwhile):
        pair = others(f"in{l}", r.in_b.at[l])
        for n in range(NX):
            q = column(n)
            for side in range(2):
                weight = r.wi[l, :, cols(side * FEAT + q * PIECE, PIECE)]
                part = jnp.dot(act, weight, preferred_element_type=F32)
                at = slice(side * PIECE, (side + 1) * PIECE)
                r.in_s[l, q, :, :, at] = part.reshape(4, BLOCK, PIECE).astype(BF16)
            reduce(pair, r.in_s.at[l], r.in_b.at[l], q)
        r.in_b[l, place] = r.in_s[l, xx, yy]
        meanwhile()
        decay = r.dec_v[l : l + 1, :]
        soft = jnp.maximum(decay, 0.0) + jnp.log1p(jnp.exp(-jnp.abs(decay)))
        soft = soft.reshape(1, 1, PIECE)

        def tap(n):
            return r.cw_v[l, n : n + 1, :].reshape(1, 1, PIECE)

        bias = r.cb_v[l : l + 1, :].reshape(1, 1, PIECE)
        early = tap(0) * r.t0_v[l] + tap(1) * r.t1_v[l] + bias
        scale = norm_scale(l)
        take(f"in{l}")
        u = (total_of(r.in_b.at[l], slice(0, PIECE)) * scale).astype(BF16).astype(F32)
        u = u.reshape(NX, ROWS, PIECE)
        v = (total_of(r.in_b.at[l], slice(PIECE, HALF)) * scale).reshape(NX, ROWS, PIECE)
        u_turned = turned(u)
        t2 = jnp.where(late3, u_turned, r.t2_v[l])
        filtered = early + tap(2) * t2 + tap(3) * u
        half = filtered.reshape(BLOCK, PIECE).astype(BF16)
        gx = jnp.dot(half, r.gxw_v[l], preferred_element_type=F32) + r.gxb_v[l : l + 1, :]
        ga = jnp.dot(half, r.gaw_v[l], preferred_element_type=F32) + r.gab_v[l : l + 1, :]
        gx = (1.0 / (1.0 + jnp.exp(-gx))).reshape(NX, ROWS, PIECE)
        ga = (1.0 / (1.0 + jnp.exp(-ga))).reshape(NX, ROWS, PIECE)
        log_a = -8.0 * ga * soft
        a = jnp.exp(log_a)
        add = jnp.sqrt(1.0 - jnp.exp(2.0 * log_a)) * (gx * filtered)
        first = a * r.st_v[l] + add
        second = a * turned(first) + add
        state = jnp.where(late3, second, first)
        gelu = 0.5 * v * (1.0 + jnp.tanh(0.7978845608028654 * (v + 0.044715 * (v * v * v))))
        r.act_s[2 * l] = (state * gelu).reshape(BLOCK, PIECE).astype(BF16)
        gather(2 * l)
        state_turned = turned(state)
        for x in range(NX):
            r.lru_s[l, x] = (state_turned[x, 0:SEQ] / scales[l]).astype(BF16)
            r.win_s[l, x, 0] = u[x, 0:SEQ].astype(BF16)
            r.win_s[l, x, 1] = u_turned[x, 0:SEQ].astype(BF16)
        give_back(l)

        merged_ready(("out", l))
        act = gathered(2 * l)
        pair = others(f"out{l}", r.out_b.at[l])
        for n in range(NX):
            q = column(n)
            part = jnp.dot(act, r.wr[l, :, cols(q * PIECE, PIECE)], preferred_element_type=F32)
            r.out_s[l, q] = part.reshape(4, BLOCK, PIECE).astype(BF16)
            reduce(pair, r.out_s.at[l], r.out_b.at[l], q)
        r.out_b[l, place] = r.out_s[l, xx, yy]
        take(f"out{l}")
        r.x_v[...] = r.x_v[...] + total_of(r.out_b.at[l], slice(0, PIECE)).reshape(NX, ROWS, PIECE)

    def next_act(k, gain):
        r.act_s[k] = (r.x_v[...].reshape(BLOCK, PIECE) * gain).astype(BF16)
        gather(k)

    merged_ready(("in", 0))
    take("rg")
    recurrent(0, (spread_in(0) * r.rgain_v[0, 0:1, :]).astype(BF16), prepare)
    next_act(1, r.rgain_v[1, 1:2, :])
    norm_send(1)
    merged_ready(("in", 1))
    recurrent(1, gathered(1), lambda: None)
    take("ag")
    next_act(3, r.again_v[...])
    norm_send(2)

    pair = sems()
    r.res_s[...] = r.x_v[...]

    def stream_send(n, _):
        x = lax.rem(xx + n, NX)
        remote(r.res_s.at[x], r.res_b.at[xx], pair, (8 * yy + 2 * x + core, j))
        return 0

    lax.fori_loop(1, NX, stream_send, 0)
    r.res_b[xx] = r.res_s[xx]
    view = r.res_b.at[pl.ds(0, NX - 1)]
    pending["stream"] = bytes_of(view, pair[1])
    pending["stream sent"] = bytes_of(view, pair[0])

    take("key", "val")
    merged_ready(("q",))
    act = gathered(3)
    pair = others("q", r.q_b)
    for n in range(4):
        at = slice(n * PIECE, (n + 1) * PIECE)
        part = jnp.dot(act, r.wq[:, at], preferred_element_type=F32)
        r.q_s[:, :, at] = part.reshape(CHIPS, ROWS, PIECE).astype(BF16)
    part = jnp.dot(act, r.wkv[...], preferred_element_type=F32)
    r.q_s[:, :, FEAT:] = part.reshape(CHIPS, ROWS, 128).astype(BF16)
    reduce_all(pair, r.q_s, r.q_b)
    scale = norm_scale(2)
    own = jnp.zeros((ROWS, 1), F32)
    for x in range(NX):
        own = jnp.where(xx == x, scale[x * ROWS : (x + 1) * ROWS], own)
    scale = own
    take("q")
    r.zsend[:, 0:FEAT] = (summed(r.q_b, slice(0, FEAT)) * scale).astype(BF16)
    kv = summed(r.q_b, slice(FEAT, FEAT + 128)) * scale
    r.zsend[:, FEAT:] = kv.astype(BF16)
    query_pair, part_pair, top_pair = sems(), sems(), sems()

    def query_send(d, _):
        remote(r.zsend, r.zbuf.at[j], query_pair, (i, lax.rem(j + d, NMP)))
        return 0

    lax.fori_loop(1, NMP, query_send, 0)
    view = r.zbuf.at[pl.ds(0, NMP - 1)]
    pending["query"] = bytes_of(view, query_pair[1])
    pending["query sent"] = bytes_of(view, query_pair[0])
    r.zbuf[j] = r.zsend[...]
    r.new_kv[0] = kv[0:SEQ].astype(BF16)
    r.new_kv[1] = pltpu.roll(kv, SEQ, 0)[0:SEQ].astype(BF16)
    take("query")

    rows = HEADS * ROWS
    query = jnp.concatenate(
        [
            r.zbuf[z, :, h * HEAD_DIM : (h + 1) * HEAD_DIM].astype(F32)
            for z in range(NMP)
            for h in range(HEADS // NMP)
        ],
        axis=0,
    ).astype(BF16)
    which = lax.broadcasted_iota(jnp.int32, (rows, SLOTS), 0) & 3
    scores = None
    for b in range(SEQ):
        one = lax.dot_general(
            query, r.key_v[b], (((1,), (1,)), ((), ())), preferred_element_type=F32
        )
        scores = one if scores is None else jnp.where(which == b, one, scores)
    mask = jnp.broadcast_to(r.mask_v[...][None], (HEADS, ROWS, SLOTS)).reshape(rows, SLOTS)
    scores = jnp.where(mask > 0.5, scores * HEAD_DIM ** (-0.5), -1e30)
    top = jnp.max(scores, axis=-1, keepdims=True)
    weight = jnp.exp(scores - top) * mask
    total = jnp.sum(weight, axis=-1, keepdims=True)
    values = None
    for b in range(SEQ):
        one = jnp.dot(
            jnp.where(which == b, weight, 0.0).astype(BF16), r.val_v[b], preferred_element_type=F32
        )
        values = one if values is None else values + one
    lane = lax.broadcasted_iota(jnp.int32, (rows, 128), 1)
    r.csend[...] = values.reshape(HEADS, ROWS, HEAD_DIM).astype(BF16)
    r.tsend[...] = jnp.where(lane < 64, top, total).reshape(HEADS, ROWS, 128)

    def part_send(d, _):
        z = lax.rem(j + d, NMP)
        group = pl.ds(4 * z, 4)
        remote(r.csend.at[group], r.cbuf.at[j], part_pair, (i, z))
        remote(r.tsend.at[group], r.tbuf.at[j], top_pair, (i, z))
        return 0

    lax.fori_loop(1, NMP, part_send, 0)
    for name, buf, pair in (("part", r.cbuf, part_pair), ("top", r.tbuf, top_pair)):
        view = buf.at[pl.ds(0, NMP - 1)]
        pending[name] = bytes_of(view, pair[1])
        pending[name + " sent"] = bytes_of(view, pair[0])
    r.cbuf[j] = r.csend[pl.ds(4 * j, 4)]
    r.tbuf[j] = r.tsend[pl.ds(4 * j, 4)]

    lateh = lax.broadcasted_iota(jnp.int32, (ROWS, HEAD_DIM), 0) >= SEQ
    late1 = lax.broadcasted_iota(jnp.int32, (ROWS, 1), 0) >= SEQ

    def pair(lo, hi):
        at = slice(FEAT, FEAT + 128)
        both = jnp.concatenate([r.zbuf[lo, :, at].astype(F32), r.zbuf[hi, :, at].astype(F32)], axis=1)
        turned = pltpu.roll(both, SEQ, 0)
        return jnp.where(lateh, turned, both), jnp.where(lateh, both, turned)

    key0, key1 = pair(0, 1)
    val0, val1 = pair(2, 3)
    fresh = []
    for h in range(4):
        head = r.zsend[:, h * HEAD_DIM : (h + 1) * HEAD_DIM].astype(F32)
        s0 = jnp.sum(head * key0, axis=-1, keepdims=True) * HEAD_DIM ** (-0.5)
        s1 = jnp.sum(head * key1, axis=-1, keepdims=True) * HEAD_DIM ** (-0.5)
        fresh.append((s0, jnp.where(late1, s1, -1e30)))
    take("part", "top")
    for h in range(4):
        s0, s1 = fresh[h]
        tops = [r.tbuf[z, h, :, 0:1] for z in range(NMP)]
        best = jnp.maximum(s0, s1)
        for t in tops:
            best = jnp.maximum(best, t)
        w0 = jnp.exp(s0 - best)
        w1 = jnp.where(late1, jnp.exp(s1 - best), 0.0)
        den = w0 + w1
        num = w0.astype(BF16).astype(F32) * val0 + w1.astype(BF16).astype(F32) * val1
        for z in range(NMP):
            fade = jnp.exp(tops[z] - best)
            den = den + fade * r.tbuf[z, h, :, 64:65]
            num = num + fade * r.cbuf[z, h].astype(F32)
        r.pieces[1, h] = (num / den).astype(BF16)
    spread(1)
    merged_ready(("o",))
    act = spread_in(1).astype(BF16)
    pair = others("o", r.o_b)
    for n in range(4):
        at = slice(n * PIECE, (n + 1) * PIECE)
        part = jnp.dot(act, r.wo[:, at], preferred_element_type=F32)
        r.o_s[:, :, at] = part.reshape(CHIPS, ROWS, PIECE).astype(BF16)
    reduce_all(pair, r.o_s, r.o_b)
    take("stream", "o")
    for q in range(NMP):
        at = slice(q * PIECE, (q + 1) * PIECE)
        x = r.res_b[q] + summed(r.o_b, at)
        r.hidden_out[0, :, at] = x[0:SEQ].astype(BF16)
        r.hidden_out[1, :, at] = pltpu.roll(x, SEQ, 0)[0:SEQ].astype(BF16)

    take(*list(pending))


def hand_over(*refs):
    for src, dst in zip(refs[:4], refs[4:]):
        dst[...] = src[...]


def body(*args):
    args = list(args)
    args[15] = args[15].reshape(1, -1)
    shape = jax.ShapeDtypeStruct
    hbm = pl.BlockSpec(memory_space=pltpu.HBM)
    vmem = pl.BlockSpec(memory_space=pltpu.VMEM)
    outs = pl.pallas_call(
        kernel,
        out_shape=(
            shape((STEPS, SEQ, FEAT), BF16),
            shape((LAYERS, SEQ, FEAT), BF16),
            shape((LAYERS, 3, SEQ, FEAT), BF16),
            shape((STEPS, SEQ, 128), BF16),
        ),
        in_specs=[hbm] * 22,
        out_specs=(vmem,) * 4,
        scratch_shapes=[kind for _, kind in scratch_list()],
        compiler_params=pltpu.CompilerParams(
            collective_id=0, has_side_effects=True, vmem_limit_bytes=VMEM
        ),
    )(*args)
    return pl.pallas_call(
        hand_over,
        out_shape=tuple(shape(out.shape, out.dtype) for out in outs),
        in_specs=[vmem] * 4,
        out_specs=(vmem,) * 4,
    )(*outs)


def solution(mesh):
    placed = (
        P(None, "dp", "mp"),
        P(),
        P(None, "dp", "mp"),
        P(None, "dp", "mp"),
        P(None, None, "mp"),
        P(None, "mp"),
        P(None, "mp", None, None),
        P(None, "mp"),
        P(None, "mp", None, None),
        P(None, "mp"),
        P(None, "mp"),
        P(None, "dp", "mp"),
        P(None, "dp", "mp"),
        P(None, None, "dp", "mp"),
        P(),
        P(),
        P("dp", "mp"),
        P("dp", "mp"),
        P("dp", "mp"),
        P("dp", "mp", None),
        P("dp", "mp", None),
        P("dp"),
    )
    return jax.shard_map(
        body,
        mesh=mesh,
        in_specs=placed,
        out_specs=(
            P(None, "dp", "mp"),
            P(None, "dp", "mp"),
            P(None, None, "dp", "mp"),
            P(None, "dp", "mp"),
        ),
        check_vma=False,
    )
```

```python
import jax
import jax.numpy as jnp
from jax import lax
from jax.experimental import pallas as pl
from jax.experimental.pallas import tpu as pltpu
from jax.sharding import PartitionSpec as P

HEADS = 16
HEAD_DIM = 256
WIN = 2048
LAYERS = 2
STEPS = 2
F32 = jnp.float32
BF16 = jnp.bfloat16
MESH = pl.DeviceIdType.MESH

NDP = 32
NMP = 4
NX = 4
ROWS = 8
SEQ = 4
FEAT = 1024
PIECE = 256
HALF = 512
SLOTS = 512
BLOCKS = 8
BLOCK = 32
CHIPS = 16
VMEM = 67043328


def scratch_list():
    V = pltpu.VMEM
    DMA = pltpu.SemaphoreType.DMA
    return [
        ("hid_v", V((STEPS, SEQ, FEAT), BF16)),
        ("rgain_v", V((2, LAYERS, PIECE), F32)),
        ("again_v", V((1, PIECE), F32)),
        ("cw_v", V((LAYERS, 4, PIECE), F32)),
        ("cb_v", V((LAYERS, PIECE), F32)),
        ("gxw_v", V((LAYERS, PIECE, PIECE), BF16)),
        ("gxb_v", V((LAYERS, PIECE), F32)),
        ("gaw_v", V((LAYERS, PIECE, PIECE), BF16)),
        ("gab_v", V((LAYERS, PIECE), F32)),
        ("dec_v", V((LAYERS, PIECE), F32)),
        ("win_v", V((LAYERS, 3, SEQ, FEAT), BF16)),
        ("key_v", V((SEQ, SLOTS, HEAD_DIM), BF16)),
        ("val_v", V((SEQ, SLOTS, HEAD_DIM), BF16)),
        ("wkv", V((PIECE, 128), BF16)),
        ("wi", V((LAYERS, PIECE, 2 * FEAT), BF16)),
        ("wr", V((LAYERS, PIECE, FEAT), BF16)),
        ("wq", V((PIECE, FEAT), BF16)),
        ("wo", V((PIECE, FEAT), BF16)),
        ("scale_s", pltpu.SMEM((LAYERS,), jnp.int32)),
        ("pos_s", pltpu.SMEM((SEQ,), jnp.int32)),
        ("x_v", V((NX, ROWS, PIECE), F32)),
        ("h_v", V((ROWS, FEAT), F32)),
        ("st_v", V((LAYERS, NX, ROWS, PIECE), F32)),
        ("t0_v", V((LAYERS, NX, ROWS, PIECE), F32)),
        ("t1_v", V((LAYERS, NX, ROWS, PIECE), F32)),
        ("t2_v", V((LAYERS, NX, ROWS, PIECE), F32)),
        ("mask_v", V((ROWS, SLOTS), F32)),
        ("lru_b", V((NX, LAYERS, SEQ, PIECE), BF16)),
        ("win_b", V((NX, LAYERS, 3, SEQ, PIECE), BF16)),
        ("lru_s", V((LAYERS, NX, SEQ, PIECE), BF16)),
        ("win_s", V((LAYERS, NX, 2, SEQ, PIECE), BF16)),
        ("pieces", V((2, NMP, ROWS, PIECE), BF16)),
        ("spread_b", V((2, CHIPS, ROWS, PIECE), BF16)),
        ("act_s", V((4, BLOCK, PIECE), BF16)),
        ("act_b", V((4, 4, BLOCK, PIECE), BF16)),
        ("in_s", V((LAYERS, NX, 4, BLOCK, HALF), BF16)),
        ("in_b", V((LAYERS, CHIPS, BLOCK, HALF), BF16)),
        ("out_s", V((LAYERS, NX, 4, BLOCK, PIECE), BF16)),
        ("out_b", V((LAYERS, CHIPS, BLOCK, PIECE), BF16)),
        ("q_s", V((CHIPS, ROWS, FEAT + 128), BF16)),
        ("q_b", V((CHIPS, ROWS, FEAT + 128), BF16)),
        ("o_s", V((CHIPS, ROWS, FEAT), BF16)),
        ("o_b", V((CHIPS, ROWS, FEAT), BF16)),
        ("ent_b", V((NX, ROWS, PIECE), BF16)),
        ("res_s", V((NX, ROWS, PIECE), F32)),
        ("res_b", V((NX, ROWS, PIECE), F32)),
        ("nsend", V((3, 1, 128), F32)),
        ("nbuf", V((3, CHIPS, 1, 128), F32)),
        ("zsend", V((ROWS, FEAT + 128), BF16)),
        ("zbuf", V((NMP, ROWS, FEAT + 128), BF16)),
        ("csend", V((HEADS, ROWS, HEAD_DIM), BF16)),
        ("cbuf", V((NMP, 4, ROWS, HEAD_DIM), BF16)),
        ("tsend", V((HEADS, ROWS, 128), F32)),
        ("tbuf", V((NMP, 4, ROWS, 128), F32)),
        ("lsem", DMA((32,))),
        ("snd", DMA((48,))),
        ("rcv", DMA((48,))),
    ]


NAMES = (
    "hidden_in",
    "rec_gain",
    "rec_in_x",
    "rec_in_y",
    "conv_weight",
    "conv_bias",
    "gate_x_weight",
    "gate_x_bias",
    "gate_a_weight",
    "gate_a_bias",
    "decay_param",
    "rec_out",
    "lru_state",
    "conv_state",
    "scale_index",
    "attn_gain",
    "attn_q",
    "attn_kv",
    "attn_out",
    "key_cache",
    "value_cache",
    "positions",
    "hidden_out",
    "lru_out",
    "conv_out",
    "new_kv",
)


class Refs:
    def __init__(self, refs):
        names = (*NAMES, *(name for name, _ in scratch_list()))
        for name, ref in zip(names, refs, strict=True):
            setattr(self, name, ref)


def kernel(*refs):
    r = Refs(refs)
    i = lax.axis_index("dp")
    j = lax.axis_index("mp")
    core = lax.rem(i, 2)
    mate = i + 1 - 2 * core
    yy = lax.div(i, 8)
    xx = lax.div(lax.rem(i, 8), 2)
    diagonal = yy == j
    place = lax.div(i, 2)

    pending = {}
    used = [0, 0]

    def take(*names):
        for name in names:
            pending.pop(name)()

    def sems():
        used[1] += 1
        assert used[1] <= 48
        return r.snd.at[used[1] - 1], r.rcv.at[used[1] - 1]

    def local(name, src, dst):
        sem = r.lsem.at[used[0]]
        used[0] += 1
        copy = pltpu.make_async_copy(src, dst, sem)
        copy.start()
        pending[name] = copy.wait

    def remote(src, dst, pair, device):
        pltpu.make_async_remote_copy(
            src_ref=src,
            dst_ref=dst,
            send_sem=pair[0],
            recv_sem=pair[1],
            device_id=device,
            device_id_type=MESH,
        ).start()

    def bytes_of(view, sem):
        return lambda: pltpu.make_async_copy(view, view, sem).wait()

    def all_but_self(buf, sem, own):
        def wait():
            @pl.when(own)
            def _():
                bytes_of(buf.at[pl.ds(0, buf.shape[0] - 1)], sem)()

            @pl.when(jnp.logical_not(own))
            def _():
                bytes_of(buf, sem)()

        return wait

    def away(here, n):
        return lax.rem(here + (2, 1, 3, 0)[n], 4)

    def cols(at, size):
        return pl.ds(pl.multiple_of(at, 128), size)

    krow = cols(core * 128, 128)
    mine = cols((4 * yy + xx) * PIECE, PIECE)
    owned = cols((4 * j + xx) * PIECE, PIECE)
    block = cols(xx * PIECE, PIECE)

    local("hid", r.hidden_in, r.hid_v)

    barrier = pltpu.get_barrier_semaphore()

    def greet(d, z):
        @pl.when(jnp.logical_not((d == i) & (z == j)))
        def _():
            pl.semaphore_signal(barrier, inc=1, device_id=(d, z), device_id_type=MESH)

    def greet_all(k, _):
        greet(2 * k + core, yy)
        greet(2 * k + core, j)
        greet(8 * yy + 2 * lax.rem(k, 4) + core, lax.div(k, 4))
        return 0

    lax.fori_loop(0, CHIPS, greet_all, 0, unroll=True)
    greet(mate, j)

    local("rg", r.rec_gain.at[:, mine], r.rgain_v.at[0])
    local("rg1", r.rec_gain.at[:, owned], r.rgain_v.at[1])
    merged = []
    for l in range(LAYERS):
        merged.append((("in", l), r.rec_in_x.at[l], r.wi.at[l, krow, pl.ds(0, FEAT)]))
        merged.append((("in", l), r.rec_in_y.at[l], r.wi.at[l, krow, pl.ds(FEAT, FEAT)]))
        merged.append((("out", l), r.rec_out.at[l], r.wr.at[l, krow, :]))
    merged.append((("q",), r.attn_q, r.wq.at[krow, :]))
    merged.append((("q",), r.attn_kv, r.wkv.at[krow, :]))
    merged.append((("o",), r.attn_out, r.wo.at[krow, :]))
    for n, (tag, src, dst) in enumerate(merged):
        local(("own", n), src, dst)
    local("cw", r.conv_weight.at[:, :, block], r.cw_v)
    local("cb", r.conv_bias.at[:, block], r.cb_v)
    local("gxb", r.gate_x_bias.at[:, block], r.gxb_v)
    local("gab", r.gate_a_bias.at[:, block], r.gab_v)
    local("dec", r.decay_param.at[:, block], r.dec_v)
    local("gxw", r.gate_x_weight.at[:, xx], r.gxw_v)
    local("gaw", r.gate_a_weight.at[:, xx], r.gaw_v)
    local("sc", r.scale_index, r.scale_s)
    local("pos", r.positions, r.pos_s)
    local("win", r.conv_state, r.win_v)
    local("ag", r.attn_gain.at[:, owned], r.again_v)
    local("key", r.key_cache, r.key_v)
    local("val", r.value_cache, r.val_v)

    late3 = lax.broadcasted_iota(jnp.int32, (NX, ROWS, PIECE), 1) >= SEQ

    def turned(values):
        return pltpu.roll(values, SEQ, 1)

    lane = lax.broadcasted_iota(jnp.int32, (BLOCK, 128), 1)
    diag = lane == lax.broadcasted_iota(jnp.int32, (BLOCK, 128), 0)

    def norm_line(k, line):
        me = NX * j + xx
        r.nsend[k] = line
        r.nbuf[k, me] = line
        pair = sems()

        def one(n, _):
            x, z = lax.div(n, NMP), lax.rem(n, NMP)

            @pl.when(jnp.logical_not((x == xx) & (z == j)))
            def _():
                remote(r.nsend.at[k], r.nbuf.at[k, me], pair, (8 * yy + 2 * x + core, z))

            return 0

        lax.fori_loop(0, CHIPS, one, 0, unroll=True)
        view = r.nbuf.at[k, pl.ds(0, CHIPS - 1)]
        pending["norm", k] = bytes_of(view, pair[1])
        pending["norm sent", k] = bytes_of(view, pair[0])

    def norm_first():
        h = r.h_v[...]
        sq = jnp.broadcast_to(jnp.sum(h * h, axis=-1, keepdims=True), (ROWS, 128))
        here = lax.broadcasted_iota(jnp.int32, (ROWS, 128), 1) - 8 * xx
        at = here == lax.broadcasted_iota(jnp.int32, (ROWS, 128), 0)
        line = jnp.sum(jnp.where(at, sq, 0.0), axis=0, keepdims=True)
        norm_line(0, line)

    def norm_send(k):
        x = r.x_v[...]
        sq = jnp.sum((x * x).reshape(BLOCK, PIECE), axis=-1, keepdims=True)
        norm_line(k, jnp.sum(jnp.where(diag, jnp.broadcast_to(sq, (BLOCK, 128)), 0.0), axis=0, keepdims=True))

    def norm_scale(k):
        take(("norm", k))
        total = r.nbuf[k, 0]
        for n in range(1, CHIPS):
            total = total + r.nbuf[k, n]
        line = lax.rsqrt(total * (1.0 / 4096.0) + 1e-06)
        return jnp.sum(jnp.where(diag, jnp.broadcast_to(line, (BLOCK, 128)), 0.0), axis=-1, keepdims=True)

    def spread(k):
        pair = sems()

        for n in range(CHIPS):
            q, z = away(xx, n // 4), away(j, n % 4)
            d = 8 * j + 2 * q + core

            @pl.when(jnp.logical_not((d == i) & (z == j)))
            def _():
                remote(r.pieces.at[k, q], r.spread_b.at[k, place], pair, (d, z))

        pending["spread", k] = all_but_self(r.spread_b.at[k], pair[1], diagonal)
        pending["spread sent", k] = all_but_self(r.spread_b.at[k], pair[0], diagonal)

        @pl.when(diagonal)
        def _():
            r.spread_b[k, place] = r.pieces[k, xx]

    def gather(k):
        pair = sems()

        for n in range(NMP):
            z = away(j, n)
            d = 8 * j + 2 * xx + core

            @pl.when(jnp.logical_not((d == i) & (z == j)))
            def _():
                remote(r.act_s.at[k], r.act_b.at[k, yy], pair, (d, z))

        pending["gather", k] = all_but_self(r.act_b.at[k], pair[1], diagonal)
        pending["gather sent", k] = all_but_self(r.act_b.at[k], pair[0], diagonal)

        @pl.when(diagonal)
        def _():
            r.act_b[k, yy] = r.act_s[k]

    def gathered(k):
        take(("gather", k))
        return r.act_b[k].reshape(4 * BLOCK, PIECE)

    def spread_in(k):
        take(("spread", k))
        return r.spread_b[k].astype(F32).reshape(4 * BLOCK, PIECE)

    def others(name, buf):
        pair = sems()
        view = buf.at[pl.ds(0, CHIPS - 1)]
        pending[name] = bytes_of(view, pair[1])
        pending[name + " sent"] = bytes_of(view, pair[0])
        return pair

    def column(n):
        return away(xx, n)

    def reduce(pair, send, buf, q, last):
        for n in range(4):
            at = away(yy, n)
            d = 8 * at + 2 * q + core

            if not (last and n == 3):
                remote(send.at[q, at], buf.at[place], pair, (d, j))

    def reduce_all(pair, send, buf):
        for n in range(CHIPS - 1):
            to = 4 * away(yy, n // 4) + away(xx, n % 4)
            remote(send.at[to], buf.at[place], pair, (2 * to + core, j))
        buf[place] = send[place]

    def total_of(buf, at):
        acc = buf[0, :, at].astype(F32)
        for n in range(1, CHIPS):
            acc = acc + buf[n, :, at].astype(F32)
        return acc

    def summed(buf, at):
        acc = buf[0, :, at].astype(F32)
        for p in range(1, CHIPS):
            acc = acc + buf[p, :, at].astype(F32)
        return acc

    take("hid")
    r.h_v[0:SEQ, :] = r.hid_v[0].astype(F32)
    r.h_v[SEQ:ROWS, :] = r.hid_v[1].astype(F32)
    for q in range(NMP):
        r.pieces[0, q] = r.h_v[:, q * PIECE : (q + 1) * PIECE].astype(BF16)

    met = 3 * CHIPS - 1
    pl.semaphore_wait(barrier, jnp.where(diagonal, met - 1, met))
    spread(0)

    def trade():
        for n, (_, src, dst) in enumerate(merged):
            pair = sems()
            remote(src, dst, pair, (mate, j))
            pending["mate", n] = bytes_of(dst, pair[1])
            pending["mate sent", n] = bytes_of(dst, pair[0])

    def merged_ready(tag):
        for n, (t, *_) in enumerate(merged):
            if t == tag:
                take(("own", n), ("mate", n))

    def states_send():
        pairs = sems(), sems(), sems()

        def one(n, _):
            x = lax.rem(xx + n, NX)
            device = (8 * yy + 2 * x + core, j)
            remote(r.pieces.at[0, x], r.ent_b.at[xx], pairs[2], device)
            remote(r.lru_state.at[:, :, cols(x * PIECE, PIECE)], r.lru_b.at[xx], pairs[0], device)
            remote(r.conv_state.at[:, :, :, cols(x * PIECE, PIECE)], r.win_b.at[xx], pairs[1], device)
            return 0

        lax.fori_loop(1, NX, one, 0, unroll=True)
        local("lru own", r.lru_state.at[:, :, block], r.lru_b.at[xx])
        local("win own", r.conv_state.at[:, :, :, block], r.win_b.at[xx])
        r.ent_b[xx] = r.pieces[0, xx]
        for name, buf, pair in (
            ("lru", r.lru_b, pairs[0]),
            ("window", r.win_b, pairs[1]),
            ("entering", r.ent_b, pairs[2]),
        ):
            view = buf.at[pl.ds(0, NX - 1)]
            pending[name] = bytes_of(view, pair[1])
            pending[name + " sent"] = bytes_of(view, pair[0])

    trade()
    norm_first()
    states_send()

    scales = []

    def prepare():
        take("pos")
        srow = lax.broadcasted_iota(jnp.int32, (ROWS, SLOTS), 0)
        slot = lax.broadcasted_iota(jnp.int32, (ROWS, SLOTS), 1) + j * SLOTS
        seq = srow & 3
        pos = jnp.where(
            seq == 0,
            r.pos_s[0],
            jnp.where(seq == 1, r.pos_s[1], jnp.where(seq == 2, r.pos_s[2], r.pos_s[3])),
        )
        step = lax.shift_right_logical(srow, 2)
        held = pos - 1 - ((pos - 1 - slot) & (WIN - 1))
        r.mask_v[...] = jnp.where((held >= 0) & (held >= pos + step - (WIN - 1)), 1.0, 0.0).astype(F32)
        take("win")
        for l in range(LAYERS):
            r.conv_out[l, 0] = r.win_v[l, 2]
        take("sc", "lru", "lru own", "window", "win own")
        for l in range(LAYERS):
            power = (r.scale_s[l].astype(F32) - 4.0) * 0.5
            scales.append(jnp.exp2(jnp.full((1, 128), power, F32))[:, :1])
            for x in range(NX):
                r.st_v[l, x, 0:SEQ, :] = r.lru_b[x, l].astype(F32) * scales[l]
                r.st_v[l, x, SEQ:ROWS, :] = jnp.zeros((SEQ, PIECE), F32)
                w0 = r.win_b[x, l, 0].astype(F32)
                w1 = r.win_b[x, l, 1].astype(F32)
                w2 = r.win_b[x, l, 2].astype(F32)
                r.t0_v[l, x, 0:SEQ, :] = w0
                r.t0_v[l, x, SEQ:ROWS, :] = w1
                r.t1_v[l, x, 0:SEQ, :] = w1
                r.t1_v[l, x, SEQ:ROWS, :] = w2
                r.t2_v[l, x, 0:SEQ, :] = w2
                r.t2_v[l, x, SEQ:ROWS, :] = jnp.zeros((SEQ, PIECE), F32)
        take("cw", "cb", "gxb", "gab", "dec", "gxw", "gaw", "rg1", "entering")
        r.x_v[...] = r.ent_b[...].astype(F32)

    def give_back(l):
        pairs = sems(), sems()

        def one(n, _):
            x = lax.rem(xx + n, NX)
            device = (8 * yy + 2 * x + core, j)
            remote(r.lru_s.at[l, x], r.lru_out.at[l, :, block], pairs[0], device)
            remote(r.win_s.at[l, x], r.conv_out.at[l, pl.ds(1, 2), :, block], pairs[1], device)
            return 0

        lax.fori_loop(1, NX, one, 0, unroll=True)
        r.lru_out[l, :, block] = r.lru_s[l, xx]
        r.conv_out[l, 1:3, :, block] = r.win_s[l, xx]
        for name, buf, pair in (("lru", r.lru_s, pairs[0]), ("window", r.win_s, pairs[1])):
            view = buf.at[l, pl.ds(0, NX - 1)]
            pending[name + " back", l] = bytes_of(view, pair[1])
            pending[name + " back sent", l] = bytes_of(view, pair[0])

    def recurrent(l, act, meanwhile):
        pair = others(f"in{l}", r.in_b.at[l])
        for n in range(NX):
            q = column(n)
            for side in range(2):
                weight = r.wi[l, :, cols(side * FEAT + q * PIECE, PIECE)]
                part = jnp.dot(act, weight, preferred_element_type=F32)
                at = slice(side * PIECE, (side + 1) * PIECE)
                r.in_s[l, q, :, :, at] = part.reshape(4, BLOCK, PIECE).astype(BF16)
            reduce(pair, r.in_s.at[l], r.in_b.at[l], q, n == NX - 1)
        r.in_b[l, place] = r.in_s[l, xx, yy]
        meanwhile()
        decay = r.dec_v[l : l + 1, :]
        soft = jnp.maximum(decay, 0.0) + jnp.log1p(jnp.exp(-jnp.abs(decay)))
        soft = soft.reshape(1, 1, PIECE)

        def tap(n):
            return r.cw_v[l, n : n + 1, :].reshape(1, 1, PIECE)

        bias = r.cb_v[l : l + 1, :].reshape(1, 1, PIECE)
        early = tap(0) * r.t0_v[l] + tap(1) * r.t1_v[l] + bias
        scale = norm_scale(l)
        take(f"in{l}")
        u = (total_of(r.in_b.at[l], slice(0, PIECE)) * scale).astype(BF16).astype(F32)
        u = u.reshape(NX, ROWS, PIECE)
        v = (total_of(r.in_b.at[l], slice(PIECE, HALF)) * scale).reshape(NX, ROWS, PIECE)
        u_turned = turned(u)
        t2 = jnp.where(late3, u_turned, r.t2_v[l])
        filtered = early + tap(2) * t2 + tap(3) * u
        half = filtered.reshape(BLOCK, PIECE).astype(BF16)
        gx = jnp.dot(half, r.gxw_v[l], preferred_element_type=F32) + r.gxb_v[l : l + 1, :]
        ga = jnp.dot(half, r.gaw_v[l], preferred_element_type=F32) + r.gab_v[l : l + 1, :]
        gx = (1.0 / (1.0 + jnp.exp(-gx))).reshape(NX, ROWS, PIECE)
        ga = (1.0 / (1.0 + jnp.exp(-ga))).reshape(NX, ROWS, PIECE)
        log_a = -8.0 * ga * soft
        a = jnp.exp(log_a)
        add = jnp.sqrt(1.0 - jnp.exp(2.0 * log_a)) * (gx * filtered)
        first = a * r.st_v[l] + add
        second = a * turned(first) + add
        state = jnp.where(late3, second, first)
        gelu = 0.5 * v * (1.0 + jnp.tanh(0.7978845608028654 * (v + 0.044715 * (v * v * v))))
        r.act_s[2 * l] = (state * gelu).reshape(BLOCK, PIECE).astype(BF16)
        gather(2 * l)
        state_turned = turned(state)
        for x in range(NX):
            r.lru_s[l, x] = (state_turned[x, 0:SEQ] / scales[l]).astype(BF16)
            r.win_s[l, x, 0] = u[x, 0:SEQ].astype(BF16)
            r.win_s[l, x, 1] = u_turned[x, 0:SEQ].astype(BF16)
        give_back(l)

        merged_ready(("out", l))
        act = gathered(2 * l)
        pair = others(f"out{l}", r.out_b.at[l])
        for n in range(NX):
            q = column(n)
            part = jnp.dot(act, r.wr[l, :, cols(q * PIECE, PIECE)], preferred_element_type=F32)
            r.out_s[l, q] = part.reshape(4, BLOCK, PIECE).astype(BF16)
            reduce(pair, r.out_s.at[l], r.out_b.at[l], q, n == NX - 1)
        r.out_b[l, place] = r.out_s[l, xx, yy]
        take(f"out{l}")
        r.x_v[...] = r.x_v[...] + total_of(r.out_b.at[l], slice(0, PIECE)).reshape(NX, ROWS, PIECE)

    def next_act(k, gain):
        r.act_s[k] = (r.x_v[...].reshape(BLOCK, PIECE) * gain).astype(BF16)
        gather(k)

    prepare()
    merged_ready(("in", 0))
    take("rg")
    recurrent(0, (spread_in(0) * r.rgain_v[0, 0:1, :]).astype(BF16), lambda: None)
    next_act(1, r.rgain_v[1, 1:2, :])
    norm_send(1)
    merged_ready(("in", 1))
    recurrent(1, gathered(1), lambda: None)
    take("ag")
    next_act(3, r.again_v[...])
    norm_send(2)

    pair = sems()
    r.res_s[...] = r.x_v[...]

    def stream_send(n, _):
        x = lax.rem(xx + n, NX)
        remote(r.res_s.at[x], r.res_b.at[xx], pair, (8 * yy + 2 * x + core, j))
        return 0

    lax.fori_loop(1, NX, stream_send, 0, unroll=True)
    r.res_b[xx] = r.res_s[xx]
    view = r.res_b.at[pl.ds(0, NX - 1)]
    pending["stream"] = bytes_of(view, pair[1])
    pending["stream sent"] = bytes_of(view, pair[0])

    take("key", "val")
    merged_ready(("q",))
    act = gathered(3)
    pair = others("q", r.q_b)
    for n in range(4):
        at = slice(n * PIECE, (n + 1) * PIECE)
        part = jnp.dot(act, r.wq[:, at], preferred_element_type=F32)
        r.q_s[:, :, at] = part.reshape(CHIPS, ROWS, PIECE).astype(BF16)
    part = jnp.dot(act, r.wkv[...], preferred_element_type=F32)
    r.q_s[:, :, FEAT:] = part.reshape(CHIPS, ROWS, 128).astype(BF16)
    reduce_all(pair, r.q_s, r.q_b)
    scale = norm_scale(2)
    own = jnp.zeros((ROWS, 1), F32)
    for x in range(NX):
        own = jnp.where(xx == x, scale[x * ROWS : (x + 1) * ROWS], own)
    scale = own
    take("q")
    r.zsend[:, 0:FEAT] = (summed(r.q_b, slice(0, FEAT)) * scale).astype(BF16)
    kv = summed(r.q_b, slice(FEAT, FEAT + 128)) * scale
    r.zsend[:, FEAT:] = kv.astype(BF16)
    query_pair, part_pair, top_pair = sems(), sems(), sems()

    def query_send(d, _):
        remote(r.zsend, r.zbuf.at[j], query_pair, (i, lax.rem(j + d, NMP)))
        return 0

    lax.fori_loop(1, NMP, query_send, 0, unroll=True)
    view = r.zbuf.at[pl.ds(0, NMP - 1)]
    pending["query"] = bytes_of(view, query_pair[1])
    pending["query sent"] = bytes_of(view, query_pair[0])
    r.zbuf[j] = r.zsend[...]
    r.new_kv[0] = kv[0:SEQ].astype(BF16)
    r.new_kv[1] = pltpu.roll(kv, SEQ, 0)[0:SEQ].astype(BF16)
    take("query")

    rows = HEADS * ROWS
    query = jnp.concatenate(
        [
            r.zbuf[z, :, h * HEAD_DIM : (h + 1) * HEAD_DIM].astype(F32)
            for z in range(NMP)
            for h in range(HEADS // NMP)
        ],
        axis=0,
    ).astype(BF16)
    which = lax.broadcasted_iota(jnp.int32, (rows, SLOTS), 0) & 3
    scores = None
    for b in range(SEQ):
        one = lax.dot_general(
            query, r.key_v[b], (((1,), (1,)), ((), ())), preferred_element_type=F32
        )
        scores = one if scores is None else jnp.where(which == b, one, scores)
    mask = jnp.broadcast_to(r.mask_v[...][None], (HEADS, ROWS, SLOTS)).reshape(rows, SLOTS)
    scores = jnp.where(mask > 0.5, scores * HEAD_DIM ** (-0.5), -1e30)
    top = jnp.max(scores, axis=-1, keepdims=True)
    weight = jnp.exp(scores - top) * mask
    total = jnp.sum(weight, axis=-1, keepdims=True)
    values = None
    for b in range(SEQ):
        one = jnp.dot(
            jnp.where(which == b, weight, 0.0).astype(BF16), r.val_v[b], preferred_element_type=F32
        )
        values = one if values is None else values + one
    lane = lax.broadcasted_iota(jnp.int32, (rows, 128), 1)
    r.csend[...] = values.reshape(HEADS, ROWS, HEAD_DIM).astype(BF16)
    r.tsend[...] = jnp.where(lane < 64, top, total).reshape(HEADS, ROWS, 128)

    def part_send(d, _):
        z = lax.rem(j + d, NMP)
        group = pl.ds(4 * z, 4)
        remote(r.csend.at[group], r.cbuf.at[j], part_pair, (i, z))
        remote(r.tsend.at[group], r.tbuf.at[j], top_pair, (i, z))
        return 0

    lax.fori_loop(1, NMP, part_send, 0, unroll=True)
    for name, buf, pair in (("part", r.cbuf, part_pair), ("top", r.tbuf, top_pair)):
        view = buf.at[pl.ds(0, NMP - 1)]
        pending[name] = bytes_of(view, pair[1])
        pending[name + " sent"] = bytes_of(view, pair[0])
    r.cbuf[j] = r.csend[pl.ds(4 * j, 4)]
    r.tbuf[j] = r.tsend[pl.ds(4 * j, 4)]

    lateh = lax.broadcasted_iota(jnp.int32, (ROWS, HEAD_DIM), 0) >= SEQ
    late1 = lax.broadcasted_iota(jnp.int32, (ROWS, 1), 0) >= SEQ

    def pair(lo, hi):
        at = slice(FEAT, FEAT + 128)
        both = jnp.concatenate([r.zbuf[lo, :, at].astype(F32), r.zbuf[hi, :, at].astype(F32)], axis=1)
        turned = pltpu.roll(both, SEQ, 0)
        return jnp.where(lateh, turned, both), jnp.where(lateh, both, turned)

    key0, key1 = pair(0, 1)
    val0, val1 = pair(2, 3)
    fresh = []
    for h in range(4):
        head = r.zsend[:, h * HEAD_DIM : (h + 1) * HEAD_DIM].astype(F32)
        s0 = jnp.sum(head * key0, axis=-1, keepdims=True) * HEAD_DIM ** (-0.5)
        s1 = jnp.sum(head * key1, axis=-1, keepdims=True) * HEAD_DIM ** (-0.5)
        fresh.append((s0, jnp.where(late1, s1, -1e30)))
    take("part", "top")
    for h in range(4):
        s0, s1 = fresh[h]
        tops = [r.tbuf[z, h, :, 0:1] for z in range(NMP)]
        best = jnp.maximum(s0, s1)
        for t in tops:
            best = jnp.maximum(best, t)
        w0 = jnp.exp(s0 - best)
        w1 = jnp.where(late1, jnp.exp(s1 - best), 0.0)
        den = w0 + w1
        num = w0.astype(BF16).astype(F32) * val0 + w1.astype(BF16).astype(F32) * val1
        for z in range(NMP):
            fade = jnp.exp(tops[z] - best)
            den = den + fade * r.tbuf[z, h, :, 64:65]
            num = num + fade * r.cbuf[z, h].astype(F32)
        r.pieces[1, h] = (num / den).astype(BF16)
    spread(1)
    merged_ready(("o",))
    act = spread_in(1).astype(BF16)
    pair = others("o", r.o_b)
    for n in range(4):
        at = slice(n * PIECE, (n + 1) * PIECE)
        part = jnp.dot(act, r.wo[:, at], preferred_element_type=F32)
        r.o_s[:, :, at] = part.reshape(CHIPS, ROWS, PIECE).astype(BF16)
    reduce_all(pair, r.o_s, r.o_b)
    take("stream", "o")
    for q in range(NMP):
        at = slice(q * PIECE, (q + 1) * PIECE)
        x = r.res_b[q] + summed(r.o_b, at)
        r.hidden_out[0, :, at] = x[0:SEQ].astype(BF16)
        r.hidden_out[1, :, at] = pltpu.roll(x, SEQ, 0)[0:SEQ].astype(BF16)

    take(*list(pending))


def hand_over(*refs):
    for src, dst in zip(refs[:4], refs[4:]):
        dst[...] = src[...]


def body(*args):
    args = list(args)
    args[15] = args[15].reshape(1, -1)
    shape = jax.ShapeDtypeStruct
    hbm = pl.BlockSpec(memory_space=pltpu.HBM)
    vmem = pl.BlockSpec(memory_space=pltpu.VMEM)
    outs = pl.pallas_call(
        kernel,
        out_shape=(
            shape((STEPS, SEQ, FEAT), BF16),
            shape((LAYERS, SEQ, FEAT), BF16),
            shape((LAYERS, 3, SEQ, FEAT), BF16),
            shape((STEPS, SEQ, 128), BF16),
        ),
        in_specs=[hbm] * 22,
        out_specs=(vmem,) * 4,
        scratch_shapes=[kind for _, kind in scratch_list()],
        compiler_params=pltpu.CompilerParams(
            collective_id=0, has_side_effects=True, vmem_limit_bytes=VMEM
        ),
    )(*args)
    return pl.pallas_call(
        hand_over,
        out_shape=tuple(shape(out.shape, out.dtype) for out in outs),
        in_specs=[vmem] * 4,
        out_specs=(vmem,) * 4,
    )(*outs)


def solution(mesh):
    placed = (
        P(None, "dp", "mp"),
        P(),
        P(None, "dp", "mp"),
        P(None, "dp", "mp"),
        P(None, None, "mp"),
        P(None, "mp"),
        P(None, "mp", None, None),
        P(None, "mp"),
        P(None, "mp", None, None),
        P(None, "mp"),
        P(None, "mp"),
        P(None, "dp", "mp"),
        P(None, "dp", "mp"),
        P(None, None, "dp", "mp"),
        P(),
        P(),
        P("dp", "mp"),
        P("dp", "mp"),
        P("dp", "mp"),
        P("dp", "mp", None),
        P("dp", "mp", None),
        P("dp"),
    )
    return jax.shard_map(
        body,
        mesh=mesh,
        in_specs=placed,
        out_specs=(
            P(None, "dp", "mp"),
            P(None, "dp", "mp"),
            P(None, None, "dp", "mp"),
            P(None, "dp", "mp"),
        ),
        check_vma=False,
    )
```

```python
import jax
import jax.numpy as jnp
from jax import lax
from jax.experimental import pallas as pl
from jax.experimental.pallas import tpu as pltpu
from jax.sharding import PartitionSpec as P

HEADS = 16
HEAD_DIM = 256
WIN = 2048
LAYERS = 2
STEPS = 2
F32 = jnp.float32
BF16 = jnp.bfloat16
MESH = pl.DeviceIdType.MESH

NDP = 32
NMP = 4
NX = 4
ROWS = 8
SEQ = 4
FEAT = 1024
PIECE = 256
HALF = 512
SLOTS = 512
BLOCKS = 8
BLOCK = 32
CHIPS = 16
ORDER = sorted(range(16), key=lambda n: -((2, 1, 1, 0)[n // 4] + (2, 1, 1, 0)[n % 4]))
VMEM = 67043328


def scratch_list():
    V = pltpu.VMEM
    DMA = pltpu.SemaphoreType.DMA
    return [
        ("hid_v", V((STEPS, SEQ, FEAT), BF16)),
        ("rgain_v", V((2, LAYERS, PIECE), F32)),
        ("again_v", V((1, PIECE), F32)),
        ("cw_v", V((LAYERS, 4, PIECE), F32)),
        ("cb_v", V((LAYERS, PIECE), F32)),
        ("gxw_v", V((LAYERS, PIECE, PIECE), BF16)),
        ("gxb_v", V((LAYERS, PIECE), F32)),
        ("gaw_v", V((LAYERS, PIECE, PIECE), BF16)),
        ("gab_v", V((LAYERS, PIECE), F32)),
        ("dec_v", V((LAYERS, PIECE), F32)),
        ("win_v", V((LAYERS, 3, SEQ, FEAT), BF16)),
        ("key_v", V((SEQ, SLOTS, HEAD_DIM), BF16)),
        ("val_v", V((SEQ, SLOTS, HEAD_DIM), BF16)),
        ("wkv", V((PIECE, 128), BF16)),
        ("wi", V((LAYERS, PIECE, 2 * FEAT), BF16)),
        ("wr", V((LAYERS, PIECE, FEAT), BF16)),
        ("wq", V((PIECE, FEAT), BF16)),
        ("wo", V((PIECE, FEAT), BF16)),
        ("scale_s", pltpu.SMEM((LAYERS,), jnp.int32)),
        ("pos_s", pltpu.SMEM((SEQ,), jnp.int32)),
        ("x_v", V((NX, ROWS, PIECE), F32)),
        ("h_v", V((ROWS, FEAT), F32)),
        ("st_v", V((LAYERS, NX, ROWS, PIECE), F32)),
        ("t0_v", V((LAYERS, NX, ROWS, PIECE), F32)),
        ("t1_v", V((LAYERS, NX, ROWS, PIECE), F32)),
        ("t2_v", V((LAYERS, NX, ROWS, PIECE), F32)),
        ("mask_v", V((ROWS, SLOTS), F32)),
        ("lru_b", V((NX, LAYERS, SEQ, PIECE), BF16)),
        ("win_b", V((NX, LAYERS, 3, SEQ, PIECE), BF16)),
        ("lru_s", V((LAYERS, NX, SEQ, PIECE), BF16)),
        ("win_s", V((LAYERS, NX, 2, SEQ, PIECE), BF16)),
        ("pieces", V((2, NMP, ROWS, PIECE), BF16)),
        ("spread_b", V((2, CHIPS, ROWS, PIECE), BF16)),
        ("act_s", V((4, BLOCK, PIECE), BF16)),
        ("act_b", V((4, 4, BLOCK, PIECE), BF16)),
        ("in_s", V((LAYERS, NX, 4, BLOCK, HALF), BF16)),
        ("in_b", V((LAYERS, CHIPS, BLOCK, HALF), BF16)),
        ("out_s", V((LAYERS, NX, 4, BLOCK, PIECE), BF16)),
        ("out_b", V((LAYERS, CHIPS, BLOCK, PIECE), BF16)),
        ("q_s", V((CHIPS, ROWS, FEAT + 128), BF16)),
        ("q_b", V((CHIPS, ROWS, FEAT + 128), BF16)),
        ("o_s", V((CHIPS, ROWS, FEAT), BF16)),
        ("o_b", V((CHIPS, ROWS, FEAT), BF16)),
        ("ent_b", V((NX, ROWS, PIECE), BF16)),
        ("res_s", V((NX, ROWS, PIECE), F32)),
        ("res_b", V((NX, ROWS, PIECE), F32)),
        ("nsend", V((3, 1, 128), F32)),
        ("nbuf", V((3, CHIPS, 1, 128), F32)),
        ("zsend", V((ROWS, FEAT + 128), BF16)),
        ("zbuf", V((NMP, ROWS, FEAT + 128), BF16)),
        ("csend", V((HEADS, ROWS, HEAD_DIM), BF16)),
        ("cbuf", V((NMP, 4, ROWS, HEAD_DIM), BF16)),
        ("tsend", V((HEADS, ROWS, 128), F32)),
        ("tbuf", V((NMP, 4, ROWS, 128), F32)),
        ("lsem", DMA((32,))),
        ("snd", DMA((48,))),
        ("rcv", DMA((48,))),
    ]


NAMES = (
    "hidden_in",
    "rec_gain",
    "rec_in_x",
    "rec_in_y",
    "conv_weight",
    "conv_bias",
    "gate_x_weight",
    "gate_x_bias",
    "gate_a_weight",
    "gate_a_bias",
    "decay_param",
    "rec_out",
    "lru_state",
    "conv_state",
    "scale_index",
    "attn_gain",
    "attn_q",
    "attn_kv",
    "attn_out",
    "key_cache",
    "value_cache",
    "positions",
    "hidden_out",
    "lru_out",
    "conv_out",
    "new_kv",
)


class Refs:
    def __init__(self, refs):
        names = (*NAMES, *(name for name, _ in scratch_list()))
        for name, ref in zip(names, refs, strict=True):
            setattr(self, name, ref)


def kernel(*refs):
    r = Refs(refs)
    i = lax.axis_index("dp")
    j = lax.axis_index("mp")
    core = lax.rem(i, 2)
    mate = i + 1 - 2 * core
    yy = lax.div(i, 8)
    xx = lax.div(lax.rem(i, 8), 2)
    diagonal = yy == j
    place = lax.div(i, 2)

    pending = {}
    used = [0, 0]

    def take(*names):
        for name in names:
            pending.pop(name)()

    def sems():
        used[1] += 1
        assert used[1] <= 48
        return r.snd.at[used[1] - 1], r.rcv.at[used[1] - 1]

    def local(name, src, dst):
        sem = r.lsem.at[used[0]]
        used[0] += 1
        copy = pltpu.make_async_copy(src, dst, sem)
        copy.start()
        pending[name] = copy.wait

    def remote(src, dst, pair, device):
        pltpu.make_async_remote_copy(
            src_ref=src,
            dst_ref=dst,
            send_sem=pair[0],
            recv_sem=pair[1],
            device_id=device,
            device_id_type=MESH,
        ).start()

    def bytes_of(view, sem):
        return lambda: pltpu.make_async_copy(view, view, sem).wait()

    def all_but_self(buf, sem, own):
        def wait():
            @pl.when(own)
            def _():
                bytes_of(buf.at[pl.ds(0, buf.shape[0] - 1)], sem)()

            @pl.when(jnp.logical_not(own))
            def _():
                bytes_of(buf, sem)()

        return wait

    def away(here, n):
        return lax.rem(here + (2, 1, 3, 0)[n], 4)

    def cols(at, size):
        return pl.ds(pl.multiple_of(at, 128), size)

    krow = cols(core * 128, 128)
    mine = cols((4 * yy + xx) * PIECE, PIECE)
    owned = cols((4 * j + xx) * PIECE, PIECE)
    block = cols(xx * PIECE, PIECE)

    local("hid", r.hidden_in, r.hid_v)

    barrier = pltpu.get_barrier_semaphore()

    def greet(d, z):
        pl.semaphore_signal(barrier, inc=1, device_id=(d, z), device_id_type=MESH)

    for n in range(CHIPS):
        d = 8 * away(yy, n // 4) + 2 * away(xx, n % 4) + core
        if n < CHIPS - 1:
            greet(d, yy)
        else:

            @pl.when(jnp.logical_not(diagonal))
            def _():
                greet(d, yy)

    for n in range(CHIPS - 1):
        greet(8 * yy + 2 * away(xx, n % 4) + core, away(j, n // 4))
        greet(8 * away(yy, n // 4) + 2 * away(xx, n % 4) + core, j)
    greet(mate, j)

    local("rg", r.rec_gain.at[:, mine], r.rgain_v.at[0])
    local("rg1", r.rec_gain.at[:, owned], r.rgain_v.at[1])
    merged = []
    for l in range(LAYERS):
        merged.append((("in", l), r.rec_in_x.at[l], r.wi.at[l, krow, pl.ds(0, FEAT)]))
        merged.append((("in", l), r.rec_in_y.at[l], r.wi.at[l, krow, pl.ds(FEAT, FEAT)]))
        merged.append((("out", l), r.rec_out.at[l], r.wr.at[l, krow, :]))
    merged.append((("q",), r.attn_q, r.wq.at[krow, :]))
    merged.append((("q",), r.attn_kv, r.wkv.at[krow, :]))
    merged.append((("o",), r.attn_out, r.wo.at[krow, :]))
    for n, (tag, src, dst) in enumerate(merged):
        local(("own", n), src, dst)
    local("cw", r.conv_weight.at[:, :, block], r.cw_v)
    local("cb", r.conv_bias.at[:, block], r.cb_v)
    local("gxb", r.gate_x_bias.at[:, block], r.gxb_v)
    local("gab", r.gate_a_bias.at[:, block], r.gab_v)
    local("dec", r.decay_param.at[:, block], r.dec_v)
    local("gxw", r.gate_x_weight.at[:, xx], r.gxw_v)
    local("gaw", r.gate_a_weight.at[:, xx], r.gaw_v)
    local("sc", r.scale_index, r.scale_s)
    local("pos", r.positions, r.pos_s)
    local("win", r.conv_state, r.win_v)
    local("ag", r.attn_gain.at[:, owned], r.again_v)
    local("key", r.key_cache, r.key_v)
    local("val", r.value_cache, r.val_v)

    late3 = lax.broadcasted_iota(jnp.int32, (NX, ROWS, PIECE), 1) >= SEQ

    def turned(values):
        return pltpu.roll(values, SEQ, 1)

    lane = lax.broadcasted_iota(jnp.int32, (BLOCK, 128), 1)
    diag = lane == lax.broadcasted_iota(jnp.int32, (BLOCK, 128), 0)

    def norm_line(k, line):
        me = NX * j + xx
        r.nsend[k] = line
        r.nbuf[k, me] = line
        pair = sems()

        def one(n, _):
            x, z = lax.div(n, NMP), lax.rem(n, NMP)

            @pl.when(jnp.logical_not((x == xx) & (z == j)))
            def _():
                remote(r.nsend.at[k], r.nbuf.at[k, me], pair, (8 * yy + 2 * x + core, z))

            return 0

        lax.fori_loop(0, CHIPS, one, 0, unroll=True)
        view = r.nbuf.at[k, pl.ds(0, CHIPS - 1)]
        pending["norm", k] = bytes_of(view, pair[1])
        pending["norm sent", k] = bytes_of(view, pair[0])

    def norm_first():
        h = r.h_v[...]
        sq = jnp.broadcast_to(jnp.sum(h * h, axis=-1, keepdims=True), (ROWS, 128))
        here = lax.broadcasted_iota(jnp.int32, (ROWS, 128), 1) - 8 * xx
        at = here == lax.broadcasted_iota(jnp.int32, (ROWS, 128), 0)
        line = jnp.sum(jnp.where(at, sq, 0.0), axis=0, keepdims=True)
        norm_line(0, line)

    def norm_send(k):
        x = r.x_v[...]
        sq = jnp.sum((x * x).reshape(BLOCK, PIECE), axis=-1, keepdims=True)
        norm_line(k, jnp.sum(jnp.where(diag, jnp.broadcast_to(sq, (BLOCK, 128)), 0.0), axis=0, keepdims=True))

    def norm_scale(k):
        take(("norm", k))
        total = r.nbuf[k, 0]
        for n in range(1, CHIPS):
            total = total + r.nbuf[k, n]
        line = lax.rsqrt(total * (1.0 / 4096.0) + 1e-06)
        return jnp.sum(jnp.where(diag, jnp.broadcast_to(line, (BLOCK, 128)), 0.0), axis=-1, keepdims=True)

    def spread(k):
        pair = sems()

        for n in range(CHIPS):
            q, z = away(xx, n // 4), away(j, n % 4)
            d = 8 * j + 2 * q + core

            @pl.when(jnp.logical_not((d == i) & (z == j)))
            def _():
                remote(r.pieces.at[k, q], r.spread_b.at[k, place], pair, (d, z))

        pending["spread", k] = all_but_self(r.spread_b.at[k], pair[1], diagonal)
        pending["spread sent", k] = all_but_self(r.spread_b.at[k], pair[0], diagonal)

        @pl.when(diagonal)
        def _():
            r.spread_b[k, place] = r.pieces[k, xx]

    def gather(k):
        pair = sems()

        for n in range(NMP):
            z = away(j, n)
            d = 8 * j + 2 * xx + core

            @pl.when(jnp.logical_not((d == i) & (z == j)))
            def _():
                remote(r.act_s.at[k], r.act_b.at[k, yy], pair, (d, z))

        pending["gather", k] = all_but_self(r.act_b.at[k], pair[1], diagonal)
        pending["gather sent", k] = all_but_self(r.act_b.at[k], pair[0], diagonal)

        @pl.when(diagonal)
        def _():
            r.act_b[k, yy] = r.act_s[k]

    def gathered(k):
        take(("gather", k))
        return r.act_b[k].reshape(4 * BLOCK, PIECE)

    def spread_in(k):
        take(("spread", k))
        return r.spread_b[k].astype(F32).reshape(4 * BLOCK, PIECE)

    def others(name, buf):
        pair = sems()
        view = buf.at[pl.ds(0, CHIPS - 1)]
        pending[name] = bytes_of(view, pair[1])
        pending[name + " sent"] = bytes_of(view, pair[0])
        return pair

    def column(n):
        return away(xx, n)

    def reduce(pair, send, buf, q, last):
        for n in range(4):
            at = away(yy, n)
            d = 8 * at + 2 * q + core

            if not (last and n == 3):
                remote(send.at[q, at], buf.at[place], pair, (d, j))

    def reduce_all(pair, send, buf):
        for n in ORDER[: CHIPS - 1]:
            to = 4 * away(yy, n // 4) + away(xx, n % 4)
            remote(send.at[to], buf.at[place], pair, (2 * to + core, j))
        buf[place] = send[place]

    def total_of(buf, at):
        acc = buf[0, :, at].astype(F32)
        for n in range(1, CHIPS):
            acc = acc + buf[n, :, at].astype(F32)
        return acc

    def summed(buf, at):
        acc = buf[0, :, at].astype(F32)
        for p in range(1, CHIPS):
            acc = acc + buf[p, :, at].astype(F32)
        return acc

    take("hid")
    r.h_v[0:SEQ, :] = r.hid_v[0].astype(F32)
    r.h_v[SEQ:ROWS, :] = r.hid_v[1].astype(F32)
    for q in range(NMP):
        r.pieces[0, q] = r.h_v[:, q * PIECE : (q + 1) * PIECE].astype(BF16)

    met = 3 * CHIPS - 1
    pl.semaphore_wait(barrier, jnp.where(diagonal, met - 1, met))
    spread(0)

    def trade():
        for n, (_, src, dst) in enumerate(merged):
            pair = sems()
            remote(src, dst, pair, (mate, j))
            pending["mate", n] = bytes_of(dst, pair[1])
            pending["mate sent", n] = bytes_of(dst, pair[0])

    def merged_ready(tag):
        for n, (t, *_) in enumerate(merged):
            if t == tag:
                take(("own", n), ("mate", n))

    def states_send():
        pairs = sems(), sems(), sems()

        def one(n, _):
            x = lax.rem(xx + n, NX)
            device = (8 * yy + 2 * x + core, j)
            remote(r.pieces.at[0, x], r.ent_b.at[xx], pairs[2], device)
            remote(r.lru_state.at[:, :, cols(x * PIECE, PIECE)], r.lru_b.at[xx], pairs[0], device)
            remote(r.conv_state.at[:, :, :, cols(x * PIECE, PIECE)], r.win_b.at[xx], pairs[1], device)
            return 0

        lax.fori_loop(1, NX, one, 0, unroll=True)
        local("lru own", r.lru_state.at[:, :, block], r.lru_b.at[xx])
        local("win own", r.conv_state.at[:, :, :, block], r.win_b.at[xx])
        r.ent_b[xx] = r.pieces[0, xx]
        for name, buf, pair in (
            ("lru", r.lru_b, pairs[0]),
            ("window", r.win_b, pairs[1]),
            ("entering", r.ent_b, pairs[2]),
        ):
            view = buf.at[pl.ds(0, NX - 1)]
            pending[name] = bytes_of(view, pair[1])
            pending[name + " sent"] = bytes_of(view, pair[0])

    trade()
    norm_first()
    states_send()

    scales = []

    def prepare():
        take("pos")
        srow = lax.broadcasted_iota(jnp.int32, (ROWS, SLOTS), 0)
        slot = lax.broadcasted_iota(jnp.int32, (ROWS, SLOTS), 1) + j * SLOTS
        seq = srow & 3
        pos = jnp.where(
            seq == 0,
            r.pos_s[0],
            jnp.where(seq == 1, r.pos_s[1], jnp.where(seq == 2, r.pos_s[2], r.pos_s[3])),
        )
        step = lax.shift_right_logical(srow, 2)
        held = pos - 1 - ((pos - 1 - slot) & (WIN - 1))
        r.mask_v[...] = jnp.where((held >= 0) & (held >= pos + step - (WIN - 1)), 1.0, 0.0).astype(F32)
        take("win")
        for l in range(LAYERS):
            r.conv_out[l, 0] = r.win_v[l, 2]
        take("sc", "lru", "lru own", "window", "win own")
        for l in range(LAYERS):
            power = (r.scale_s[l].astype(F32) - 4.0) * 0.5
            scales.append(jnp.exp2(jnp.full((1, 128), power, F32))[:, :1])
            for x in range(NX):
                r.st_v[l, x, 0:SEQ, :] = r.lru_b[x, l].astype(F32) * scales[l]
                r.st_v[l, x, SEQ:ROWS, :] = jnp.zeros((SEQ, PIECE), F32)
                w0 = r.win_b[x, l, 0].astype(F32)
                w1 = r.win_b[x, l, 1].astype(F32)
                w2 = r.win_b[x, l, 2].astype(F32)
                r.t0_v[l, x, 0:SEQ, :] = w0
                r.t0_v[l, x, SEQ:ROWS, :] = w1
                r.t1_v[l, x, 0:SEQ, :] = w1
                r.t1_v[l, x, SEQ:ROWS, :] = w2
                r.t2_v[l, x, 0:SEQ, :] = w2
                r.t2_v[l, x, SEQ:ROWS, :] = jnp.zeros((SEQ, PIECE), F32)
        take("cw", "cb", "gxb", "gab", "dec", "gxw", "gaw", "rg1", "entering")
        r.x_v[...] = r.ent_b[...].astype(F32)

    def give_back(l):
        pairs = sems(), sems()

        def one(n, _):
            x = lax.rem(xx + n, NX)
            device = (8 * yy + 2 * x + core, j)
            remote(r.lru_s.at[l, x], r.lru_out.at[l, :, block], pairs[0], device)
            remote(r.win_s.at[l, x], r.conv_out.at[l, pl.ds(1, 2), :, block], pairs[1], device)
            return 0

        lax.fori_loop(1, NX, one, 0, unroll=True)
        r.lru_out[l, :, block] = r.lru_s[l, xx]
        r.conv_out[l, 1:3, :, block] = r.win_s[l, xx]
        for name, buf, pair in (("lru", r.lru_s, pairs[0]), ("window", r.win_s, pairs[1])):
            view = buf.at[l, pl.ds(0, NX - 1)]
            pending[name + " back", l] = bytes_of(view, pair[1])
            pending[name + " back sent", l] = bytes_of(view, pair[0])

    def recurrent(l, act, meanwhile):
        pair = others(f"in{l}", r.in_b.at[l])
        for n in range(NX):
            q = column(n)
            for side in range(2):
                weight = r.wi[l, :, cols(side * FEAT + q * PIECE, PIECE)]
                part = jnp.dot(act, weight, preferred_element_type=F32)
                at = slice(side * PIECE, (side + 1) * PIECE)
                r.in_s[l, q, :, :, at] = part.reshape(4, BLOCK, PIECE).astype(BF16)
            reduce(pair, r.in_s.at[l], r.in_b.at[l], q, n == NX - 1)
        r.in_b[l, place] = r.in_s[l, xx, yy]
        meanwhile()
        decay = r.dec_v[l : l + 1, :]
        soft = jnp.maximum(decay, 0.0) + jnp.log1p(jnp.exp(-jnp.abs(decay)))
        soft = soft.reshape(1, 1, PIECE)

        def tap(n):
            return r.cw_v[l, n : n + 1, :].reshape(1, 1, PIECE)

        bias = r.cb_v[l : l + 1, :].reshape(1, 1, PIECE)
        early = tap(0) * r.t0_v[l] + tap(1) * r.t1_v[l] + bias
        scale = norm_scale(l)
        take(f"in{l}")
        u = (total_of(r.in_b.at[l], slice(0, PIECE)) * scale).astype(BF16).astype(F32)
        u = u.reshape(NX, ROWS, PIECE)
        v = (total_of(r.in_b.at[l], slice(PIECE, HALF)) * scale).reshape(NX, ROWS, PIECE)
        u_turned = turned(u)
        t2 = jnp.where(late3, u_turned, r.t2_v[l])
        filtered = early + tap(2) * t2 + tap(3) * u
        half = filtered.reshape(BLOCK, PIECE).astype(BF16)
        gx = jnp.dot(half, r.gxw_v[l], preferred_element_type=F32) + r.gxb_v[l : l + 1, :]
        ga = jnp.dot(half, r.gaw_v[l], preferred_element_type=F32) + r.gab_v[l : l + 1, :]
        gx = (1.0 / (1.0 + jnp.exp(-gx))).reshape(NX, ROWS, PIECE)
        ga = (1.0 / (1.0 + jnp.exp(-ga))).reshape(NX, ROWS, PIECE)
        log_a = -8.0 * ga * soft
        a = jnp.exp(log_a)
        add = jnp.sqrt(1.0 - jnp.exp(2.0 * log_a)) * (gx * filtered)
        first = a * r.st_v[l] + add
        second = a * turned(first) + add
        state = jnp.where(late3, second, first)
        gelu = 0.5 * v * (1.0 + jnp.tanh(0.7978845608028654 * (v + 0.044715 * (v * v * v))))
        r.act_s[2 * l] = (state * gelu).reshape(BLOCK, PIECE).astype(BF16)
        gather(2 * l)
        state_turned = turned(state)
        for x in range(NX):
            r.lru_s[l, x] = (state_turned[x, 0:SEQ] / scales[l]).astype(BF16)
            r.win_s[l, x, 0] = u[x, 0:SEQ].astype(BF16)
            r.win_s[l, x, 1] = u_turned[x, 0:SEQ].astype(BF16)
        give_back(l)

        merged_ready(("out", l))
        act = gathered(2 * l)
        pair = others(f"out{l}", r.out_b.at[l])
        for n in range(NX):
            q = column(n)
            part = jnp.dot(act, r.wr[l, :, cols(q * PIECE, PIECE)], preferred_element_type=F32)
            r.out_s[l, q] = part.reshape(4, BLOCK, PIECE).astype(BF16)
            reduce(pair, r.out_s.at[l], r.out_b.at[l], q, n == NX - 1)
        r.out_b[l, place] = r.out_s[l, xx, yy]
        take(f"out{l}")
        r.x_v[...] = r.x_v[...] + total_of(r.out_b.at[l], slice(0, PIECE)).reshape(NX, ROWS, PIECE)

    def next_act(k, gain):
        r.act_s[k] = (r.x_v[...].reshape(BLOCK, PIECE) * gain).astype(BF16)
        gather(k)

    prepare()
    merged_ready(("in", 0))
    take("rg")
    recurrent(0, (spread_in(0) * r.rgain_v[0, 0:1, :]).astype(BF16), lambda: None)
    next_act(1, r.rgain_v[1, 1:2, :])
    norm_send(1)
    merged_ready(("in", 1))
    recurrent(1, gathered(1), lambda: None)
    take("ag")
    next_act(3, r.again_v[...])
    norm_send(2)

    pair = sems()
    r.res_s[...] = r.x_v[...]

    def stream_send(n, _):
        x = lax.rem(xx + n, NX)
        remote(r.res_s.at[x], r.res_b.at[xx], pair, (8 * yy + 2 * x + core, j))
        return 0

    lax.fori_loop(1, NX, stream_send, 0, unroll=True)
    r.res_b[xx] = r.res_s[xx]
    view = r.res_b.at[pl.ds(0, NX - 1)]
    pending["stream"] = bytes_of(view, pair[1])
    pending["stream sent"] = bytes_of(view, pair[0])

    take("key", "val")
    merged_ready(("q",))
    act = gathered(3)
    pair = others("q", r.q_b)
    for n in range(4):
        at = slice(n * PIECE, (n + 1) * PIECE)
        part = jnp.dot(act, r.wq[:, at], preferred_element_type=F32)
        r.q_s[:, :, at] = part.reshape(CHIPS, ROWS, PIECE).astype(BF16)
    part = jnp.dot(act, r.wkv[...], preferred_element_type=F32)
    r.q_s[:, :, FEAT:] = part.reshape(CHIPS, ROWS, 128).astype(BF16)
    reduce_all(pair, r.q_s, r.q_b)
    scale = norm_scale(2)
    own = jnp.zeros((ROWS, 1), F32)
    for x in range(NX):
        own = jnp.where(xx == x, scale[x * ROWS : (x + 1) * ROWS], own)
    scale = own
    take("q")
    r.zsend[:, 0:FEAT] = (summed(r.q_b, slice(0, FEAT)) * scale).astype(BF16)
    kv = summed(r.q_b, slice(FEAT, FEAT + 128)) * scale
    r.zsend[:, FEAT:] = kv.astype(BF16)
    query_pair, part_pair, top_pair = sems(), sems(), sems()

    def query_send(d, _):
        remote(r.zsend, r.zbuf.at[j], query_pair, (i, lax.rem(j + d, NMP)))
        return 0

    lax.fori_loop(1, NMP, query_send, 0, unroll=True)
    view = r.zbuf.at[pl.ds(0, NMP - 1)]
    pending["query"] = bytes_of(view, query_pair[1])
    pending["query sent"] = bytes_of(view, query_pair[0])
    r.zbuf[j] = r.zsend[...]
    r.new_kv[0] = kv[0:SEQ].astype(BF16)
    r.new_kv[1] = pltpu.roll(kv, SEQ, 0)[0:SEQ].astype(BF16)
    take("query")

    rows = HEADS * ROWS
    query = jnp.concatenate(
        [
            r.zbuf[z, :, h * HEAD_DIM : (h + 1) * HEAD_DIM].astype(F32)
            for z in range(NMP)
            for h in range(HEADS // NMP)
        ],
        axis=0,
    ).astype(BF16)
    which = lax.broadcasted_iota(jnp.int32, (rows, SLOTS), 0) & 3
    scores = None
    for b in range(SEQ):
        one = lax.dot_general(
            query, r.key_v[b], (((1,), (1,)), ((), ())), preferred_element_type=F32
        )
        scores = one if scores is None else jnp.where(which == b, one, scores)
    mask = jnp.broadcast_to(r.mask_v[...][None], (HEADS, ROWS, SLOTS)).reshape(rows, SLOTS)
    scores = jnp.where(mask > 0.5, scores * HEAD_DIM ** (-0.5), -1e30)
    top = jnp.max(scores, axis=-1, keepdims=True)
    weight = jnp.exp(scores - top) * mask
    total = jnp.sum(weight, axis=-1, keepdims=True)
    values = None
    for b in range(SEQ):
        one = jnp.dot(
            jnp.where(which == b, weight, 0.0).astype(BF16), r.val_v[b], preferred_element_type=F32
        )
        values = one if values is None else values + one
    lane = lax.broadcasted_iota(jnp.int32, (rows, 128), 1)
    r.csend[...] = values.reshape(HEADS, ROWS, HEAD_DIM).astype(BF16)
    r.tsend[...] = jnp.where(lane < 64, top, total).reshape(HEADS, ROWS, 128)

    def part_send(d, _):
        z = lax.rem(j + d, NMP)
        group = pl.ds(4 * z, 4)
        remote(r.csend.at[group], r.cbuf.at[j], part_pair, (i, z))
        remote(r.tsend.at[group], r.tbuf.at[j], top_pair, (i, z))
        return 0

    lax.fori_loop(1, NMP, part_send, 0, unroll=True)
    for name, buf, pair in (("part", r.cbuf, part_pair), ("top", r.tbuf, top_pair)):
        view = buf.at[pl.ds(0, NMP - 1)]
        pending[name] = bytes_of(view, pair[1])
        pending[name + " sent"] = bytes_of(view, pair[0])
    r.cbuf[j] = r.csend[pl.ds(4 * j, 4)]
    r.tbuf[j] = r.tsend[pl.ds(4 * j, 4)]

    lateh = lax.broadcasted_iota(jnp.int32, (ROWS, HEAD_DIM), 0) >= SEQ
    late1 = lax.broadcasted_iota(jnp.int32, (ROWS, 1), 0) >= SEQ

    def pair(lo, hi):
        at = slice(FEAT, FEAT + 128)
        both = jnp.concatenate([r.zbuf[lo, :, at].astype(F32), r.zbuf[hi, :, at].astype(F32)], axis=1)
        turned = pltpu.roll(both, SEQ, 0)
        return jnp.where(lateh, turned, both), jnp.where(lateh, both, turned)

    key0, key1 = pair(0, 1)
    val0, val1 = pair(2, 3)
    fresh = []
    for h in range(4):
        head = r.zsend[:, h * HEAD_DIM : (h + 1) * HEAD_DIM].astype(F32)
        s0 = jnp.sum(head * key0, axis=-1, keepdims=True) * HEAD_DIM ** (-0.5)
        s1 = jnp.sum(head * key1, axis=-1, keepdims=True) * HEAD_DIM ** (-0.5)
        fresh.append((s0, jnp.where(late1, s1, -1e30)))
    take("part", "top")
    for h in range(4):
        s0, s1 = fresh[h]
        tops = [r.tbuf[z, h, :, 0:1] for z in range(NMP)]
        best = jnp.maximum(s0, s1)
        for t in tops:
            best = jnp.maximum(best, t)
        w0 = jnp.exp(s0 - best)
        w1 = jnp.where(late1, jnp.exp(s1 - best), 0.0)
        den = w0 + w1
        num = w0.astype(BF16).astype(F32) * val0 + w1.astype(BF16).astype(F32) * val1
        for z in range(NMP):
            fade = jnp.exp(tops[z] - best)
            den = den + fade * r.tbuf[z, h, :, 64:65]
            num = num + fade * r.cbuf[z, h].astype(F32)
        r.pieces[1, h] = (num / den).astype(BF16)
    spread(1)
    merged_ready(("o",))
    act = spread_in(1).astype(BF16)
    pair = others("o", r.o_b)
    for n in range(4):
        at = slice(n * PIECE, (n + 1) * PIECE)
        part = jnp.dot(act, r.wo[:, at], preferred_element_type=F32)
        r.o_s[:, :, at] = part.reshape(CHIPS, ROWS, PIECE).astype(BF16)
    reduce_all(pair, r.o_s, r.o_b)
    take("stream", "o")
    for q in range(NMP):
        at = slice(q * PIECE, (q + 1) * PIECE)
        x = r.res_b[q] + summed(r.o_b, at)
        r.hidden_out[0, :, at] = x[0:SEQ].astype(BF16)
        r.hidden_out[1, :, at] = pltpu.roll(x, SEQ, 0)[0:SEQ].astype(BF16)

    take(*list(pending))


def hand_over(*refs):
    for src, dst in zip(refs[:4], refs[4:]):
        dst[...] = src[...]


def body(*args):
    args = list(args)
    args[15] = args[15].reshape(1, -1)
    shape = jax.ShapeDtypeStruct
    hbm = pl.BlockSpec(memory_space=pltpu.HBM)
    vmem = pl.BlockSpec(memory_space=pltpu.VMEM)
    outs = pl.pallas_call(
        kernel,
        out_shape=(
            shape((STEPS, SEQ, FEAT), BF16),
            shape((LAYERS, SEQ, FEAT), BF16),
            shape((LAYERS, 3, SEQ, FEAT), BF16),
            shape((STEPS, SEQ, 128), BF16),
        ),
        in_specs=[hbm] * 22,
        out_specs=(vmem,) * 4,
        scratch_shapes=[kind for _, kind in scratch_list()],
        compiler_params=pltpu.CompilerParams(
            collective_id=0, has_side_effects=True, vmem_limit_bytes=VMEM
        ),
    )(*args)
    return pl.pallas_call(
        hand_over,
        out_shape=tuple(shape(out.shape, out.dtype) for out in outs),
        in_specs=[vmem] * 4,
        out_specs=(vmem,) * 4,
    )(*outs)


def solution(mesh):
    placed = (
        P(None, "dp", "mp"),
        P(),
        P(None, "dp", "mp"),
        P(None, "dp", "mp"),
        P(None, None, "mp"),
        P(None, "mp"),
        P(None, "mp", None, None),
        P(None, "mp"),
        P(None, "mp", None, None),
        P(None, "mp"),
        P(None, "mp"),
        P(None, "dp", "mp"),
        P(None, "dp", "mp"),
        P(None, None, "dp", "mp"),
        P(),
        P(),
        P("dp", "mp"),
        P("dp", "mp"),
        P("dp", "mp"),
        P("dp", "mp", None),
        P("dp", "mp", None),
        P("dp"),
    )
    return jax.shard_map(
        body,
        mesh=mesh,
        in_specs=placed,
        out_specs=(
            P(None, "dp", "mp"),
            P(None, "dp", "mp"),
            P(None, None, "dp", "mp"),
            P(None, "dp", "mp"),
        ),
        check_vma=False,
    )
```
